256 devices in a mesh: blk: 128 (over z, x, y), rep: 2 (over core).
Axes of the slice: x: 4, y: 4, z: 8, core: 2. Of those that a mesh axis runs over, the one named last changes fastest.
Arguments:
- points: float32 [128, 3, 8192], P('blk'), may hold values from -6 to 6
- normals: float32 [128, 3, 8192], P('blk'), may hold values from -6 to 6
- src_block: int32 [8, 128, 1, 16], P(None, 'blk', None, 'rep'), may hold values from 0 to 63
- tgt_index: int32 [8, 128, 1, 16, 128], P(None, 'blk', None, 'rep'), may hold values from 0 to 8191
- active: int32 [8, 128, 1], P(None, 'blk'), may hold values from 0 to 16
Outputs:
- diag_hess: float32 [128, 36], P('blk')
- gradient: float32 [128, 6], P('blk')
- pair_hess: float32 [8, 128, 1, 36], P(None, 'blk')
The draws below stay inside these ranges and needn't reach their ends.
Inputs may be any that keep to these rules, and one draw needn't show every extreme that they name: Slots j with j >= active contribute nothing.
All inputs are finite; a program needn't handle non-finite values.
Results may differ from the reference program's by a relative error of at most 0.00017.
Values sent between devices are 32-bit elements; how exact they have to be, the bound alone decides.
A program may use at most 64 MiB of HBM per device.

```python
import jax
import jax.numpy as jnp
from jax import lax

SC = 1
P_SIZE = 8192
NB = 16
BLOCK = 128
ROUNDS = 8
NSCANS = 128
N_BLK = 128


def place_ends(values, key, low, high):
    longest = values.shape.index(max(values.shape))
    spots = []
    for shift in (0, 1):
        where = [jax.random.randint(jax.random.fold_in(key, axis), (), 0, length) for axis, length in enumerate(values.shape)]
        where[longest] = (where[longest] + shift) % values.shape[longest]
        spots.append(tuple(where))
    return values.at[spots[0]].set(low).at[spots[1]].set(high)


def level_of(rng, extent, shards, low, high):
    level = 1.0
    for dim, shards_of in shards:
        steps = jax.random.uniform(jax.random.fold_in(jax.random.fold_in(rng, 6), dim), (shards_of,), jnp.float32, low / len(shards), high / len(shards))
        level = level * jnp.repeat(jnp.exp(steps), extent[dim] // shards_of).reshape((-1,) + (1,) * (len(extent) - 1 - dim))
    return level


def gaussian(key, extent, width, limit, pieces=(), kind=jnp.bfloat16):
    gain = level_of(key, extent, pieces, -0.22, 0.18) if pieces else 1.0
    drawn = jax.random.normal(key, extent, jnp.float32) * width * gain
    return jnp.minimum(jnp.maximum(drawn, -limit), limit).astype(kind)


def setup_inputs(seed: int = 0) -> dict:
    key_of = jax.random.split(jax.random.key(seed), 6)
    return {
        "points": gaussian(key_of[0], (NSCANS, 3, P_SIZE), 0.5, 6.0, ((0, 128),), jnp.float32),
        "normals": gaussian(key_of[1], (NSCANS, 3, P_SIZE), 1.0, 6.0, ((0, 128),), jnp.float32),
        "src_block": place_ends(jax.random.randint(key_of[2], (ROUNDS, NSCANS, SC, NB), 0, P_SIZE // BLOCK), jax.random.fold_in(key_of[2], 1), 0, (P_SIZE // BLOCK) - 1).astype(jnp.int32),
        "tgt_index": place_ends(jax.random.randint(key_of[3], (ROUNDS, NSCANS, SC, NB, BLOCK), 0, P_SIZE), jax.random.fold_in(key_of[3], 1), 0, P_SIZE - 1).astype(jnp.int32),
        "active": place_ends(jax.random.randint(key_of[4], (ROUNDS, NSCANS, SC), 0, NB + 1), jax.random.fold_in(key_of[4], 1), 0, NB).astype(jnp.int32),
    }


def reference(points, normals, src_block, tgt_index, active):
    nscans = points.shape[0]
    npts = points.shape[2]
    slots = NB * BLOCK
    flat_p = jnp.moveaxis(points, 1, 0).reshape(3, -1)
    flat_n = jnp.moveaxis(normals, 1, 0).reshape(3, -1)
    lanes = jnp.arange(BLOCK, dtype=jnp.int32)
    owner = jnp.arange(nscans, dtype=jnp.int32) // SC
    local = jnp.arange(SC, dtype=jnp.int32)
    scans = jnp.arange(nscans, dtype=jnp.int32)
    slot_block = jnp.arange(slots, dtype=jnp.int32) // BLOCK
    diag = jnp.zeros((nscans, 36), jnp.float32)
    grad = jnp.zeros((nscans, 6), jnp.float32)
    pairs = []
    for k in range(1, ROUNDS + 1):
        tscan = (((owner[:, None] - k) % N_BLK) * SC + local[None, :]).astype(jnp.int32)
        sidx = (scans[:, None, None, None] * npts + src_block[k - 1][:, :, :, None] * BLOCK + lanes).reshape(nscans, SC, slots)
        tidx = tscan[:, :, None] * npts + tgt_index[k - 1].reshape(nscans, SC, slots)
        p = flat_p[:, sidx]
        q = flat_p[:, tidx]
        n = flat_n[:, tidx]
        live = (slot_block[None, None, :] < active[k - 1][:, :, None]).astype(jnp.float32)
        resid = jnp.sum(n * (p - q), axis=0)
        weight = live / (1.0 + resid * resid)
        jacob = jnp.stack([p[1] * n[2] - p[2] * n[1], p[2] * n[0] - p[0] * n[2], p[0] * n[1] - p[1] * n[0], n[0], n[1], n[2]])
        gram = jnp.einsum('iast,jast->asij', jacob * weight, jacob, precision=lax.Precision.HIGHEST) / (NB * BLOCK)
        push = jnp.einsum('iast,ast->asi', jacob, weight * resid, precision=lax.Precision.HIGHEST) / (NB * BLOCK)
        gram = gram.reshape(nscans, SC, 36)
        pairs.append(gram)
        diag = diag + gram.sum(1)
        grad = grad + push.sum(1)
        diag = diag.at[tscan.reshape(-1)].add(gram.reshape(-1, 36))
        grad = grad.at[tscan.reshape(-1)].add(-push.reshape(-1, 6))
    scale = 2.0 * ROUNDS * SC
    return diag / scale, grad / scale, jnp.stack(pairs)
```

```python
import functools

import jax
import jax.numpy as jnp
from jax import lax
from jax.experimental import pallas as pl
from jax.experimental.pallas import tpu as pltpu
from jax.sharding import PartitionSpec as P

BLOCK = 128
PLANE = 16
CHUNKS = 2
MESH = pl.DeviceIdType.MESH


def kernel(
    n, reps, pts_hbm, nrm_hbm, src_hbm, tgt_hbm, act_hbm, out,
    pts, nrm, low_pts, low_nrm, src, tgt, act, stage, inbox, part, prod, res, got, own, other,
    low_sum, high_sum,
    load, out_send, out_recv, back_send, back_recv, pair_send, pair_recv,
    push_send, push_recv, low_send, low_recv, low_go,
):
    rounds, per_rep = tgt.shape[0], tgt.shape[3]
    rows = pts.shape[1]
    span = rows // CHUNKS
    npts = rows * BLOCK
    me = lax.axis_index("blk")
    half = lax.axis_index("rep")
    partner = 1 - half
    spot = lax.rem(me, PLANE)
    base = me - spot
    above = lax.rem(me + PLANE, n)
    below = lax.rem(me + n - PLANE, n)
    wraps = spot >= PLANE - rounds
    n_own = jnp.minimum(rounds, PLANE - 1 - spot)

    def peer(d):
        return base + lax.rem(spot + d, PLANE)

    loads = [
        pltpu.make_async_copy(a, b, load.at[i])
        for i, (a, b) in enumerate(
            ((src_hbm, src), (act_hbm, act), (tgt_hbm, tgt), (pts_hbm, pts), (nrm_hbm, nrm))
        )
    ]
    for copy in loads:
        copy.start()

    barrier = pltpu.get_barrier_semaphore()
    for d in range(1, PLANE):
        for r in range(reps):
            pl.semaphore_signal(
                barrier, inc=1, device_id={"blk": peer(d), "rep": r}, device_id_type=MESH
            )
    for r in range(reps):
        pl.semaphore_signal(
            barrier, inc=1, device_id={"blk": below, "rep": r}, device_id_type=MESH
        )
    pl.semaphore_signal(barrier, inc=1, device_id={"blk": me, "rep": partner}, device_id_type=MESH)

    prod[...] = jnp.zeros_like(prod)
    res[...] = jnp.zeros_like(res)
    for copy in loads[:4]:
        copy.wait()

    slot = lax.broadcasted_iota(jnp.int32, (per_rep, BLOCK), 0) + half * per_rep
    for k in range(rounds):
        for j in range(per_rep):
            block = src[k, 0, 0, j]
            for c in range(3):
                stage[k, c * per_rep + j, :] = pts[c, block]
        index = jnp.where(slot < act[0, k], tgt[k, 0, 0], npts)
        stage[k, 3 * per_rep :, :] = index.astype(jnp.float32)
    loads[4].wait()

    pl.semaphore_wait(barrier, (PLANE - 1) * reps + reps + 1)

    def outgoing(k):
        return pltpu.make_async_remote_copy(
            src_ref=stage.at[k],
            dst_ref=inbox.at[k],
            send_sem=out_send.at[k],
            recv_sem=out_recv.at[k],
            device_id={"blk": peer(PLANE - 1 - k), "rep": half},
            device_id_type=MESH,
        )

    def returned(k, r):
        return pltpu.make_async_remote_copy(
            src_ref=res.at[k + 1],
            dst_ref=got.at[k, half],
            send_sem=back_send.at[k, r],
            recv_sem=back_recv.at[k, half],
            device_id={"blk": peer(k + 1), "rep": r},
            device_id_type=MESH,
        )

    def arrival(k, r):
        return pltpu.make_async_remote_copy(
            src_ref=res.at[k + 1],
            dst_ref=got.at[k, r],
            send_sem=back_send.at[k, r],
            recv_sem=back_recv.at[k, r],
            device_id={"blk": peer(k + 1), "rep": r},
            device_id_type=MESH,
        )

    def push(c, i):
        a, b = ((pts, low_pts), (nrm, low_nrm))[i]
        return pltpu.make_async_remote_copy(
            src_ref=a.at[:, c * span : (c + 1) * span, :],
            dst_ref=b.at[c],
            send_sem=push_send.at[c, i],
            recv_sem=push_recv.at[c, i],
            device_id={"blk": above, "rep": half},
            device_id_type=MESH,
        )

    def lowered(r):
        return pltpu.make_async_remote_copy(
            src_ref=low_sum,
            dst_ref=high_sum.at[half],
            send_sem=low_send.at[r],
            recv_sem=low_recv.at[half],
            device_id={"blk": below, "rep": r},
            device_id_type=MESH,
        )

    def raised(r):
        return pltpu.make_async_remote_copy(
            src_ref=low_sum,
            dst_ref=high_sum.at[r],
            send_sem=low_send.at[r],
            recv_sem=low_recv.at[r],
            device_id={"blk": below, "rep": r},
            device_id_type=MESH,
        )

    for k in range(rounds):
        outgoing(k).start()

    @pl.when(wraps)
    def _():
        for c in range(CHUNKS):
            for i in range(2):
                push(c, i).start()
        for r in range(reps):
            pl.semaphore_signal(
                low_go, inc=1, device_id={"blk": above, "rep": r}, device_id_type=MESH
            )

    def look_up(k, first, count, line_of, found):
        index = inbox[k, 3 * per_rep :, :].astype(jnp.int32)
        lane = index & (BLOCK - 1)
        row = index >> (BLOCK.bit_length() - 1)
        for h in range(count):
            here = row == first + h
            for c in range(6):
                line = jnp.broadcast_to(line_of(c, h), (per_rep, BLOCK))
                value = jnp.take_along_axis(line, lane, axis=1, mode="promise_in_bounds")
                found[c] = jnp.where(here, value, found[c])
        return found

    def terms(k, found):
        p = [inbox[k, c * per_rep : (c + 1) * per_rep, :] for c in range(3)]
        q, m = found[:3], found[3:]
        resid = m[0] * (p[0] - q[0]) + m[1] * (p[1] - q[1]) + m[2] * (p[2] - q[2])
        weight = 1.0 / (1.0 + resid * resid)
        jacob = [
            p[1] * m[2] - p[2] * m[1],
            p[2] * m[0] - p[0] * m[2],
            p[0] * m[1] - p[1] * m[0],
            m[0],
            m[1],
            m[2],
        ]
        for i in range(6):
            scaled = jacob[i] * weight
            for j in range(i, 6):
                line = jnp.sum(scaled * jacob[j], axis=0, keepdims=True)
                prod[k + 1, 6 * i + j : 6 * i + j + 1, :] = line
                if j != i:
                    prod[k + 1, 6 * j + i : 6 * j + i + 1, :] = line
            prod[k + 1, 36 + i : 37 + i, :] = jnp.sum(scaled * resid, axis=0, keepdims=True)

    width = prod.shape[1]
    ones = jnp.ones((8, BLOCK), jnp.float32)

    def lane_sums(k):
        sums = lax.dot_general(
            ones, prod[k + 1], (((1,), (1,)), ((), ())),
            precision=lax.Precision.HIGHEST, preferred_element_type=jnp.float32,
        )
        res[k + 1, :, :width] = sums[:1] / (reps * per_rep * BLOCK)

    def send_back(k):
        for r in range(reps):
            returned(k, r).start()

    def empty():
        return [jnp.zeros((per_rep, BLOCK), jnp.float32) for _ in range(6)]

    def own_round(k, carry):
        outgoing(k).wait_recv()
        lane_sums(k - 1)
        terms(k, look_up(
            k, 0, rows, lambda c, h: (pts if c < 3 else nrm)[c % 3, h : h + 1, :], empty()
        ))

        @pl.when(k > 0)
        def _():
            send_back(k - 1)

        return carry

    lax.fori_loop(0, n_own, own_round, 0)

    @pl.when(n_own > 0)
    def _():
        lane_sums(n_own - 1)
        send_back(n_own - 1)

    @pl.when(wraps)
    def _():
        for chunk in range(CHUNKS):
            for i in range(2):
                push(chunk, i).wait_recv()
            last = chunk == CHUNKS - 1

            def low_round(k, carry, chunk=chunk, last=last):
                if chunk == 0:
                    outgoing(k).wait_recv()
                if last:

                    @pl.when(k > n_own)
                    def _():
                        lane_sums(k - 1)

                found = empty() if chunk == 0 else [part[k, c] for c in range(6)]
                found = look_up(
                    k, chunk * span, span,
                    lambda c, h: (low_pts if c < 3 else low_nrm)[chunk, c % 3, h : h + 1, :],
                    found,
                )
                if last:
                    terms(k, found)

                    @pl.when(k > n_own)
                    def _():
                        send_back(k - 1)
                else:
                    for c in range(6):
                        part[k, c] = found[c]
                return carry

            lax.fori_loop(n_own, rounds, low_round, 0)
        lane_sums(rounds - 1)
        send_back(rounds - 1)

    lanes = lax.broadcasted_iota(jnp.int32, (1, BLOCK), 1)
    sign = jnp.where(lanes < 36, 1.0, -1.0)
    total = jnp.zeros((1, BLOCK), jnp.float32)
    lower = jnp.zeros((1, BLOCK), jnp.float32)
    for k in range(rounds):
        mine = k < n_own
        total = total + jnp.where(mine, res[k + 1], 0.0)
        lower = lower + jnp.where(mine, 0.0, res[k + 1])
    own[...] = total * sign
    swap = pltpu.make_async_remote_copy(
        src_ref=own,
        dst_ref=other,
        send_sem=pair_send,
        recv_sem=pair_recv,
        device_id={"blk": me, "rep": partner},
        device_id_type=MESH,
    )
    swap.start()

    @pl.when(wraps)
    def _():
        low_sum[...] = lower * sign
        pl.semaphore_wait(low_go, reps)
        for r in range(reps):
            lowered(r).start()

    for k in range(rounds):
        outgoing(k).wait_send()
    swap.wait()
    total = own[...] + other[...]
    for k in range(rounds):
        for r in range(reps):
            arrival(k, r).wait_recv()
        both = got[k, 0] + got[k, 1]
        out[k : k + 1, :] = both
        total = total + both
    own[...] = total

    @pl.when(wraps)
    def _():
        for r in range(reps):
            raised(r).wait_recv()
        own[...] = own[...] + high_sum[0] + high_sum[1]

    out[rounds : rounds + 1, :] = own[...] / (2.0 * rounds)
    for k in range(rounds):
        for r in range(reps):
            returned(k, r).wait_send()

    @pl.when(wraps)
    def _():
        for c in range(CHUNKS):
            for i in range(2):
                push(c, i).wait_send()
        for r in range(reps):
            lowered(r).wait_send()


def split(sums, diag_ref, grad_ref, pair_ref):
    rounds = pair_ref.shape[0]
    for k in range(rounds):
        pair_ref[k, 0] = sums[k : k + 1, :36]
    diag_ref[...] = sums[rounds : rounds + 1, :36]
    grad_ref[...] = sums[rounds : rounds + 1, 36:42]


def by_rows(scan):
    return jnp.moveaxis(scan, 1, 0).reshape(scan.shape[1], -1, BLOCK)


def body(n, reps, points, normals, src_block, tgt_index, active):
    rounds, count = src_block.shape[:2]
    per_rep = src_block.shape[3]
    if count != 1 or reps != 2 or n % PLANE or n <= PLANE or rounds > PLANE // 2:
        raise ValueError("unsupported sizes")
    vmem = pl.BlockSpec(memory_space=pltpu.VMEM)
    f32, i32 = jnp.float32, jnp.int32
    rows = points.shape[2] // BLOCK
    dma = pltpu.SemaphoreType.DMA
    sums = pl.pallas_call(
        functools.partial(kernel, n, reps),
        out_shape=pltpu.VMEM((rounds + 1, BLOCK), f32),
        in_specs=[pl.BlockSpec(memory_space=pl.ANY)] * 5,
        out_specs=vmem,
        scratch_shapes=[
            pltpu.VMEM((3, rows, BLOCK), f32),
            pltpu.VMEM((3, rows, BLOCK), f32),
            pltpu.VMEM((CHUNKS, 3, rows // CHUNKS, BLOCK), f32),
            pltpu.VMEM((CHUNKS, 3, rows // CHUNKS, BLOCK), f32),
            pltpu.SMEM(src_block.shape, i32),
            pltpu.VMEM(tgt_index.shape, i32),
            pltpu.SMEM((1, rounds), i32),
            pltpu.VMEM((rounds, 4 * per_rep, BLOCK), f32),
            pltpu.VMEM((rounds, 4 * per_rep, BLOCK), f32),
            pltpu.VMEM((rounds, 6, per_rep, BLOCK), f32),
            pltpu.VMEM((rounds + 1, 48, BLOCK), f32),
            pltpu.VMEM((rounds + 1, 1, BLOCK), f32),
            pltpu.VMEM((rounds, reps, 1, BLOCK), f32),
            pltpu.VMEM((1, BLOCK), f32),
            pltpu.VMEM((1, BLOCK), f32),
            pltpu.VMEM((1, BLOCK), f32),
            pltpu.VMEM((reps, 1, BLOCK), f32),
            dma((5,)),
            dma((rounds,)),
            dma((rounds,)),
            dma((rounds, reps)),
            dma((rounds, reps)),
            dma,
            dma,
            dma((CHUNKS, 2)),
            dma((CHUNKS, 2)),
            dma((reps,)),
            dma((reps,)),
            pltpu.SemaphoreType.REGULAR,
        ],
        compiler_params=pltpu.CompilerParams(collective_id=0, has_side_effects=True),
        name="normal_equations",
    )(by_rows(points), by_rows(normals), src_block, tgt_index, active.reshape(1, rounds))
    return pl.pallas_call(
        split,
        out_shape=(
            jax.ShapeDtypeStruct((1, 36), f32),
            jax.ShapeDtypeStruct((1, 6), f32),
            jax.ShapeDtypeStruct((rounds, 1, 1, 36), f32),
        ),
        in_specs=[vmem],
        out_specs=(vmem, vmem, vmem),
        name="split_sums",
    )(pltpu.with_memory_space_constraint(sums, pltpu.VMEM))


def solution(mesh):
    return jax.shard_map(
        functools.partial(body, mesh.shape["blk"], mesh.shape["rep"]),
        mesh=mesh,
        in_specs=(
            P("blk", None, None),
            P("blk", None, None),
            P(None, "blk", None, "rep"),
            P(None, "blk", None, "rep", None),
            P(None, "blk", None),
        ),
        out_specs=(P("blk", None), P("blk", None), P(None, "blk", None, None)),
        check_vma=False,
    )
```

```python
import functools

import jax
import jax.numpy as jnp
from jax import lax
from jax.experimental import pallas as pl
from jax.experimental.pallas import tpu as pltpu
from jax.sharding import PartitionSpec as P

BLOCK = 128
PLANE = 16
CHUNKS = 2
MESH = pl.DeviceIdType.MESH


def kernel(
    n, reps, pts_hbm, nrm_hbm, src_hbm, tgt_hbm, act_hbm, out,
    pts, tab, src, tgt, act, stage, inbox, part, prod, res, got, own, other, low_sum, high_sum,
    load, fill, out_send, out_recv, back_send, back_recv, pair_send, pair_recv,
    push_send, push_recv, low_send, low_recv, low_go, back_go,
):
    rounds, per_rep = tgt.shape[0], tgt.shape[3]
    rows = pts.shape[1]
    span = rows // CHUNKS
    npts = rows * BLOCK
    me = lax.axis_index("blk")
    half = lax.axis_index("rep")
    partner = 1 - half
    spot = lax.rem(me, PLANE)
    base = me - spot
    above = lax.rem(me + PLANE, n)
    below = lax.rem(me + n - PLANE, n)
    wraps = spot >= PLANE - rounds
    n_own = jnp.minimum(rounds, PLANE - 1 - spot)

    def peer(d):
        return base + lax.rem(spot + d, PLANE)

    barrier = pltpu.get_barrier_semaphore()
    for d in range(rounds, 0, -1):
        for r in range(reps):
            pl.semaphore_signal(
                barrier, inc=1, device_id={"blk": peer(d), "rep": r}, device_id_type=MESH
            )
    for r in range(reps):
        pl.semaphore_signal(
            barrier, inc=1, device_id={"blk": below, "rep": r}, device_id_type=MESH
        )
    pl.semaphore_signal(barrier, inc=1, device_id={"blk": me, "rep": partner}, device_id_type=MESH)

    loads = [
        pltpu.make_async_copy(a, b, load.at[i])
        for i, (a, b) in enumerate(((src_hbm, src), (act_hbm, act), (tgt_hbm, tgt), (pts_hbm, pts)))
    ]
    fills = [
        pltpu.make_async_copy(
            a.at[:, c * span : (c + 1) * span, :], tab.at[0, c, 3 * i : 3 * i + 3], fill
        )
        for c in range(CHUNKS)
        for i, a in enumerate((pts_hbm, nrm_hbm))
    ]
    for copy in loads + fills:
        copy.start()

    prod[...] = jnp.zeros_like(prod)
    res[...] = jnp.zeros_like(res)
    inbox[0:2] = jnp.zeros((2, *inbox.shape[1:]), jnp.float32)
    part[0:2] = jnp.zeros((2, *part.shape[1:]), jnp.float32)
    for copy in loads:
        copy.wait()

    slot = lax.broadcasted_iota(jnp.int32, (per_rep, BLOCK), 0) + half * per_rep
    for k in range(rounds):
        for j in range(per_rep):
            block = src[k, 0, 0, j]
            for c in range(3):
                stage[k, c * per_rep + j, :] = pts[c, block]
        index = jnp.where(slot < act[0, k], tgt[k, 0, 0], npts)
        stage[k, 3 * per_rep :, :] = index.astype(jnp.float32)
    pltpu.make_async_copy(tab.at[1], tab.at[0], fill).wait()

    pl.semaphore_wait(barrier, rounds * reps + reps + 1)

    def outgoing(k):
        return pltpu.make_async_remote_copy(
            src_ref=stage.at[k],
            dst_ref=inbox.at[k + 2],
            send_sem=out_send,
            recv_sem=out_recv.at[k // 2],
            device_id={"blk": peer(PLANE - 1 - k), "rep": half},
            device_id_type=MESH,
        )

    def incoming(first):
        return pltpu.make_async_remote_copy(
            src_ref=stage.at[0:2],
            dst_ref=inbox.at[pl.ds(first, 2)],
            send_sem=out_send,
            recv_sem=out_recv.at[first // 2 - 1],
            device_id={"blk": above, "rep": half},
            device_id_type=MESH,
        )

    def returned(k, r):
        return pltpu.make_async_remote_copy(
            src_ref=res.at[k + 2],
            dst_ref=got.at[k, half],
            send_sem=back_send,
            recv_sem=back_recv,
            device_id={"blk": peer(k + 1), "rep": r},
            device_id_type=MESH,
        )

    def arrivals():
        return pltpu.make_async_remote_copy(
            src_ref=got,
            dst_ref=got,
            send_sem=back_send,
            recv_sem=back_recv,
            device_id={"blk": above, "rep": half},
            device_id_type=MESH,
        )

    def push(c):
        return pltpu.make_async_remote_copy(
            src_ref=tab.at[0, c],
            dst_ref=tab.at[1, c],
            send_sem=push_send,
            recv_sem=push_recv.at[c],
            device_id={"blk": above, "rep": half},
            device_id_type=MESH,
        )

    def lowered(r):
        return pltpu.make_async_remote_copy(
            src_ref=low_sum,
            dst_ref=high_sum.at[half],
            send_sem=low_send,
            recv_sem=low_recv,
            device_id={"blk": below, "rep": r},
            device_id_type=MESH,
        )

    def raised():
        return pltpu.make_async_remote_copy(
            src_ref=high_sum,
            dst_ref=high_sum,
            send_sem=low_send,
            recv_sem=low_recv,
            device_id={"blk": below, "rep": half},
            device_id_type=MESH,
        )

    @pl.when(wraps)
    def _():
        for c in range(CHUNKS):
            push(c).start()

    for k in range(rounds):
        outgoing(k).start()
    for k in range(rounds):
        pl.semaphore_signal(
            back_go, inc=1,
            device_id={"blk": peer(PLANE - 1 - k), "rep": partner}, device_id_type=MESH,
        )

    @pl.when(wraps)
    def _():
        for r in range(reps):
            pl.semaphore_signal(
                low_go, inc=1, device_id={"blk": above, "rep": r}, device_id_type=MESH
            )

    def look_up(first, chunks, fresh):
        lane, row, side, found = [], [], [], []
        for u in range(2):
            index = inbox[first + u, 3 * per_rep :, :].astype(jnp.int32)
            lane.append(index & (BLOCK - 1))
            row.append(index >> (BLOCK.bit_length() - 1))
            side.append(jnp.where(first + u - 2 < n_own, 0, 1))
            found.append([
                jnp.zeros((per_rep, BLOCK), jnp.float32) if fresh else part[first + u, c]
                for c in range(6)
            ])
        for u in range(2):
            for chunk in chunks:
                for h in range(span):
                    here = row[u] == chunk * span + h
                    for c in range(6):
                        line = tab[side[u], chunk, c, h : h + 1, :]
                        line = jnp.broadcast_to(line, (per_rep, BLOCK))
                        value = jnp.take_along_axis(line, lane[u], axis=1, mode="promise_in_bounds")
                        found[u][c] = jnp.where(here, value, found[u][c])
        for u in range(2):
            for c in range(6):
                part[first + u, c] = found[u][c]

    width = prod.shape[1]
    ones = jnp.ones((8, BLOCK), jnp.float32)

    def terms(k):
        p = [inbox[k, c * per_rep : (c + 1) * per_rep, :] for c in range(3)]
        q = [part[k, c] for c in range(3)]
        m = [part[k, c] for c in range(3, 6)]
        resid = m[0] * (p[0] - q[0]) + m[1] * (p[1] - q[1]) + m[2] * (p[2] - q[2])
        weight = 1.0 / (1.0 + resid * resid)
        jacob = [
            p[1] * m[2] - p[2] * m[1],
            p[2] * m[0] - p[0] * m[2],
            p[0] * m[1] - p[1] * m[0],
            m[0],
            m[1],
            m[2],
        ]
        for i in range(6):
            scaled = jacob[i] * weight
            for j in range(i, 6):
                line = jnp.sum(scaled * jacob[j], axis=0, keepdims=True)
                prod[k, 6 * i + j : 6 * i + j + 1, :] = line
                if j != i:
                    prod[k, 6 * j + i : 6 * j + i + 1, :] = line
            prod[k, 36 + i : 37 + i, :] = jnp.sum(scaled * resid, axis=0, keepdims=True)

    def finish(first):
        for u in range(2):
            terms(first + u)
        for u in range(2):
            sums = lax.dot_general(
                ones, prod[first + u], (((1,), (1,)), ((), ())),
                precision=lax.Precision.HIGHEST, preferred_element_type=jnp.float32,
            )
            res[first + u, :, :width] = sums[:1] / (reps * per_rep * BLOCK)

    def send_back(first):
        for u in range(2):
            k = first + u - 2
            for r in range(reps):
                returned(k, r).start()

    def wait_pair(first):
        incoming(first).wait_recv()

    everything = range(CHUNKS)
    pairs = rounds // 2
    own_pairs = n_own // 2
    turns = jnp.logical_and(me < PLANE, own_pairs == 0)

    def low_at(i):
        turned = jnp.where(i == 0, 0, jnp.where(i == pairs - 1, 1, i + 1))
        return jnp.where(turns, turned, own_pairs + i)

    def own_pair(i, carry):
        first = 2 * i + 2
        wait_pair(first)
        finish(first - 2)
        look_up(first, everything, True)

        @pl.when(i == 0)
        def _():
            pl.semaphore_wait(back_go, rounds)

        @pl.when(i > 0)
        def _():
            send_back(first - 2)

        return carry

    lax.fori_loop(0, own_pairs, own_pair, 0)

    @pl.when(own_pairs > 0)
    def _():
        finish(2 * own_pairs)
        send_back(2 * own_pairs)

    @pl.when(own_pairs == 0)
    def _():
        pl.semaphore_wait(back_go, rounds)

    @pl.when(wraps)
    def _():
        push(0).wait_recv()

        def low_first(i, carry):
            first = 2 * low_at(i) + 2
            wait_pair(first)
            look_up(first, [0], True)
            return carry

        lax.fori_loop(0, pairs - own_pairs, low_first, 0)
        for chunk in range(1, CHUNKS - 1):
            push(chunk).wait_recv()

            def low_next(i, carry, chunk=chunk):
                look_up(2 * low_at(i) + 2, [chunk], False)
                return carry

            lax.fori_loop(0, pairs - own_pairs, low_next, 0)
        push(CHUNKS - 1).wait_recv()

        start = 2 * own_pairs + 2
        look_up(start, [CHUNKS - 1], False)
        finish(start)
        send_back(start)

        def low_last(i, carry):
            before = jnp.where(i > 1, 2 * low_at(i - 1) + 2, 0)
            finish(before)
            look_up(2 * low_at(i) + 2, [CHUNKS - 1], False)

            @pl.when(i > 1)
            def _():
                send_back(before)

            return carry

        lax.fori_loop(1, pairs - own_pairs, low_last, 0)

        @pl.when(pairs - own_pairs > 1)
        def _():
            final = 2 * low_at(pairs - own_pairs - 1) + 2
            finish(final)
            send_back(final)

    lanes = lax.broadcasted_iota(jnp.int32, (1, BLOCK), 1)
    sign = jnp.where(lanes < 36, 1.0, -1.0)
    total = jnp.zeros((1, BLOCK), jnp.float32)
    lower = jnp.zeros((1, BLOCK), jnp.float32)
    for k in range(rounds):
        mine = k < n_own
        total = total + jnp.where(mine, res[k + 2], 0.0)
        lower = lower + jnp.where(mine, 0.0, res[k + 2])
    own[...] = total * sign
    swap = pltpu.make_async_remote_copy(
        src_ref=own,
        dst_ref=other,
        send_sem=pair_send,
        recv_sem=pair_recv,
        device_id={"blk": me, "rep": partner},
        device_id_type=MESH,
    )
    swap.start()

    @pl.when(wraps)
    def _():
        low_sum[...] = lower * sign
        pl.semaphore_wait(low_go, reps)
        for r in range(reps):
            lowered(r).start()

    pltpu.make_async_remote_copy(
        src_ref=stage,
        dst_ref=inbox.at[0:rounds],
        send_sem=out_send,
        recv_sem=out_recv.at[0],
        device_id={"blk": above, "rep": half},
        device_id_type=MESH,
    ).wait_send()

    @pl.when(wraps)
    def _():
        pltpu.make_async_remote_copy(
            src_ref=tab.at[0],
            dst_ref=tab.at[1],
            send_sem=push_send,
            recv_sem=push_recv.at[0],
            device_id={"blk": above, "rep": half},
            device_id_type=MESH,
        ).wait_send()
        raised().wait_send()

    arrivals().wait_send()
    swap.wait()
    total = own[...] + other[...]
    arrivals().wait_recv()
    for k in range(rounds):
        both = got[k, 0] + got[k, 1]
        out[k : k + 1, :] = both
        total = total + both
    own[...] = total

    @pl.when(wraps)
    def _():
        raised().wait_recv()
        own[...] = own[...] + high_sum[0] + high_sum[1]

    out[rounds : rounds + 1, :] = own[...] / (2.0 * rounds)


def split(sums, diag_ref, grad_ref, pair_ref):
    rounds = pair_ref.shape[0]
    for k in range(rounds):
        pair_ref[k, 0] = sums[k : k + 1, :36]
    diag_ref[...] = sums[rounds : rounds + 1, :36]
    grad_ref[...] = sums[rounds : rounds + 1, 36:42]


def by_rows(scan):
    return jnp.moveaxis(scan, 1, 0).reshape(scan.shape[1], -1, BLOCK)


def body(n, reps, points, normals, src_block, tgt_index, active):
    rounds, count = src_block.shape[:2]
    per_rep = src_block.shape[3]
    if count != 1 or reps != 2 or n % PLANE or n <= PLANE or rounds > PLANE // 2 or rounds % 2:
        raise ValueError("unsupported sizes")
    vmem = pl.BlockSpec(memory_space=pltpu.VMEM)
    f32, i32 = jnp.float32, jnp.int32
    rows = points.shape[2] // BLOCK
    dma = pltpu.SemaphoreType.DMA
    sums = pl.pallas_call(
        functools.partial(kernel, n, reps),
        out_shape=pltpu.VMEM((rounds + 1, BLOCK), f32),
        in_specs=[pl.BlockSpec(memory_space=pl.ANY)] * 5,
        out_specs=vmem,
        scratch_shapes=[
            pltpu.VMEM((3, rows, BLOCK), f32),
            pltpu.VMEM((2, CHUNKS, 6, rows // CHUNKS, BLOCK), f32),
            pltpu.SMEM(src_block.shape, i32),
            pltpu.VMEM(tgt_index.shape, i32),
            pltpu.SMEM((1, rounds), i32),
            pltpu.VMEM((rounds, 4 * per_rep, BLOCK), f32),
            pltpu.VMEM((rounds + 2, 4 * per_rep, BLOCK), f32),
            pltpu.VMEM((rounds + 2, 6, per_rep, BLOCK), f32),
            pltpu.VMEM((rounds + 2, 48, BLOCK), f32),
            pltpu.VMEM((rounds + 2, 1, BLOCK), f32),
            pltpu.VMEM((rounds, reps, 1, BLOCK), f32),
            pltpu.VMEM((1, BLOCK), f32),
            pltpu.VMEM((1, BLOCK), f32),
            pltpu.VMEM((1, BLOCK), f32),
            pltpu.VMEM((reps, 1, BLOCK), f32),
            dma((4,)),
            dma,
            dma,
            dma((rounds // 2,)),
            dma,
            dma,
            dma,
            dma,
            dma,
            dma((CHUNKS,)),
            dma,
            dma,
            pltpu.SemaphoreType.REGULAR,
            pltpu.SemaphoreType.REGULAR,
        ],
        compiler_params=pltpu.CompilerParams(collective_id=0, has_side_effects=True),
        name="normal_equations",
    )(by_rows(points), by_rows(normals), src_block, tgt_index, active.reshape(1, rounds))
    return pl.pallas_call(
        split,
        out_shape=(
            jax.ShapeDtypeStruct((1, 36), f32),
            jax.ShapeDtypeStruct((1, 6), f32),
            jax.ShapeDtypeStruct((rounds, 1, 1, 36), f32),
        ),
        in_specs=[vmem],
        out_specs=(vmem, vmem, vmem),
        name="split_sums",
    )(pltpu.with_memory_space_constraint(sums, pltpu.VMEM))


def solution(mesh):
    return jax.shard_map(
        functools.partial(body, mesh.shape["blk"], mesh.shape["rep"]),
        mesh=mesh,
        in_specs=(
            P("blk", None, None),
            P("blk", None, None),
            P(None, "blk", None, "rep"),
            P(None, "blk", None, "rep", None),
            P(None, "blk", None),
        ),
        out_specs=(P("blk", None), P("blk", None), P(None, "blk", None, None)),
        check_vma=False,
    )
```

```python
import functools

import jax
import jax.numpy as jnp
from jax import lax
from jax.experimental import pallas as pl
from jax.experimental.pallas import tpu as pltpu
from jax.sharding import PartitionSpec as P

BLOCK = 128
PLANE = 16
CHUNKS = 2
MESH = pl.DeviceIdType.MESH


def kernel(
    n, reps, pts_hbm, nrm_hbm, src_hbm, tgt_hbm, act_hbm, out,
    pts, tab, cut, src, tgt, act, stage, inbox, part, prod, res, got, own, other, low_sum, high_sum,
    load, fill, out_send, out_recv, back_send, back_recv, pair_send, pair_recv,
    push_send, push_recv, share_recv, low_send, low_recv, low_go, back_go,
):
    rounds, per_rep = tgt.shape[0], tgt.shape[3]
    rows = pts.shape[1]
    span = rows // CHUNKS
    npts = rows * BLOCK
    me = lax.axis_index("blk")
    half = lax.axis_index("rep")
    partner = 1 - half
    spot = lax.rem(me, PLANE)
    base = me - spot
    above = lax.rem(me + PLANE, n)
    below = lax.rem(me + n - PLANE, n)
    wraps = spot >= PLANE - rounds
    n_own = jnp.minimum(rounds, PLANE - 1 - spot)

    def peer(d):
        return base + lax.rem(spot + d, PLANE)

    sub = lax.broadcasted_iota(jnp.int32, (per_rep, BLOCK), 0)

    def split_table(side):
        for c in range(3):
            for chunk in range(CHUNKS):
                value = tab[side, chunk, 3 + c]
                lanes = slice(chunk * BLOCK, (chunk + 1) * BLOCK)
                for piece in range(3):
                    high = value.astype(jnp.bfloat16).astype(jnp.float32)
                    at = (3 * piece + c) * span
                    cut[side, at : at + span, lanes] = high
                    value = value - high

    barrier = pltpu.get_barrier_semaphore()
    for d in range(rounds, 0, -1):
        for r in range(reps):
            pl.semaphore_signal(
                barrier, inc=1, device_id={"blk": peer(d), "rep": r}, device_id_type=MESH
            )
    for r in range(reps):
        pl.semaphore_signal(
            barrier, inc=1, device_id={"blk": below, "rep": r}, device_id_type=MESH
        )
    pl.semaphore_signal(barrier, inc=1, device_id={"blk": me, "rep": partner}, device_id_type=MESH)

    loads = [
        pltpu.make_async_copy(a, b, load.at[i])
        for i, (a, b) in enumerate(((src_hbm, src), (act_hbm, act), (tgt_hbm, tgt), (pts_hbm, pts)))
    ]
    fills = [
        pltpu.make_async_copy(
            a.at[:, c * span : (c + 1) * span, :], tab.at[0, c, 3 * i : 3 * i + 3], fill
        )
        for c in range(CHUNKS)
        for i, a in enumerate((pts_hbm, nrm_hbm))
    ]
    for copy in loads + fills:
        copy.start()

    prod[...] = jnp.zeros_like(prod)
    res[...] = jnp.zeros_like(res)
    inbox[0:2] = jnp.zeros((2, *inbox.shape[1:]), jnp.float32)
    part[0:2] = jnp.zeros((2, *part.shape[1:]), jnp.float32)
    for copy in loads:
        copy.wait()

    slot = lax.broadcasted_iota(jnp.int32, (per_rep, BLOCK), 0) + half * per_rep
    for k in range(rounds):
        for j in range(per_rep):
            block = src[k, 0, 0, j]
            for c in range(3):
                stage[k, c * per_rep + j, :] = pts[c, block]
        index = jnp.where(slot < act[0, k], tgt[k, 0, 0], npts)
        stage[k, 3 * per_rep :, :] = index.astype(jnp.float32)
    pltpu.make_async_copy(tab.at[1], tab.at[0], fill).wait()

    split_table(0)
    pl.semaphore_wait(barrier, rounds * reps + reps + 1)

    def outgoing(k):
        return pltpu.make_async_remote_copy(
            src_ref=stage.at[k],
            dst_ref=inbox.at[k + 2],
            send_sem=out_send,
            recv_sem=out_recv.at[k // 2],
            device_id={"blk": peer(PLANE - 1 - k), "rep": half},
            device_id_type=MESH,
        )

    def incoming(first):
        return pltpu.make_async_remote_copy(
            src_ref=stage.at[0:2],
            dst_ref=inbox.at[pl.ds(first, 2)],
            send_sem=out_send,
            recv_sem=out_recv.at[first // 2 - 1],
            device_id={"blk": above, "rep": half},
            device_id_type=MESH,
        )

    def returned(k, r):
        return pltpu.make_async_remote_copy(
            src_ref=res.at[k + 2],
            dst_ref=got.at[k, half],
            send_sem=back_send,
            recv_sem=back_recv,
            device_id={"blk": peer(k + 1), "rep": r},
            device_id_type=MESH,
        )

    def arrivals():
        return pltpu.make_async_remote_copy(
            src_ref=got,
            dst_ref=got,
            send_sem=back_send,
            recv_sem=back_recv,
            device_id={"blk": above, "rep": half},
            device_id_type=MESH,
        )

    def push(c):
        return pltpu.make_async_remote_copy(
            src_ref=tab.at[0, c, pl.ds(3 * half, 3)],
            dst_ref=tab.at[1, c, pl.ds(3 * half, 3)],
            send_sem=push_send,
            recv_sem=push_recv.at[c],
            device_id={"blk": above, "rep": half},
            device_id_type=MESH,
        )

    def share(c, at):
        return pltpu.make_async_remote_copy(
            src_ref=tab.at[1, c, pl.ds(3 * at, 3)],
            dst_ref=tab.at[1, c, pl.ds(3 * at, 3)],
            send_sem=push_send,
            recv_sem=share_recv,
            device_id={"blk": me, "rep": partner},
            device_id_type=MESH,
        )

    def lowered(r):
        return pltpu.make_async_remote_copy(
            src_ref=low_sum,
            dst_ref=high_sum.at[half],
            send_sem=low_send,
            recv_sem=low_recv,
            device_id={"blk": below, "rep": r},
            device_id_type=MESH,
        )

    def raised():
        return pltpu.make_async_remote_copy(
            src_ref=high_sum,
            dst_ref=high_sum,
            send_sem=low_send,
            recv_sem=low_recv,
            device_id={"blk": below, "rep": half},
            device_id_type=MESH,
        )

    @pl.when(wraps)
    def _():
        for c in range(CHUNKS):
            push(c).start()

    for k in range(rounds):
        outgoing(k).start()
    for k in range(rounds):
        pl.semaphore_signal(
            back_go, inc=1,
            device_id={"blk": peer(PLANE - 1 - k), "rep": partner}, device_id_type=MESH,
        )

    @pl.when(wraps)
    def _():
        for r in range(reps):
            pl.semaphore_signal(
                low_go, inc=1, device_id={"blk": above, "rep": r}, device_id_type=MESH
            )

    def look_up_lanes(first):
        lane, row, side, found = [], [], [], []
        for u in range(2):
            index = inbox[first + u, 3 * per_rep :, :].astype(jnp.int32)
            lane.append(index & (BLOCK - 1))
            row.append(index >> (BLOCK.bit_length() - 1))
            side.append(jnp.where(first + u - 2 < n_own, 0, 1))
            found.append([jnp.zeros((per_rep, BLOCK), jnp.float32) for c in range(3)])
        for u in range(2):
            for chunk in range(CHUNKS):
                for h in range(span):
                    here = row[u] == chunk * span + h
                    for c in range(3):
                        line = tab[side[u], chunk, c, h : h + 1, :]
                        line = jnp.broadcast_to(line, (per_rep, BLOCK))
                        value = jnp.take_along_axis(line, lane[u], axis=1, mode="promise_in_bounds")
                        found[u][c] = jnp.where(here, value, found[u][c])
        for u in range(2):
            for c in range(3):
                part[first + u, c] = found[u][c]

    def look_up_dot(first):
        for u in range(2):
            side = jnp.where(first + u - 2 < n_own, 0, 1)
            for s in range(0, per_rep, 2):
                hot, group = [], []
                for v in range(2):
                    at = 3 * per_rep + s + v
                    line = jnp.broadcast_to(inbox[first + u, at : at + 1, :], (per_rep, BLOCK))
                    line = line.astype(jnp.int32)
                    row = line >> (BLOCK.bit_length() - 1)
                    column = (line & (BLOCK - 1)) + (row >> (span.bit_length() - 1)) * BLOCK - sub
                    group.append((row & (span - 1)) - sub)
                    hot.append(jnp.concatenate([
                        jnp.where(column == i, 1.0, 0.0)
                        for i in range(0, CHUNKS * BLOCK, per_rep)
                    ], axis=0))
                picked = lax.dot_general(
                    cut[side], jnp.concatenate(hot, axis=1), (((1,), (0,)), ((), ())),
                    precision=lax.Precision.DEFAULT, preferred_element_type=jnp.float32,
                )
                picked = picked[: 3 * span] + picked[3 * span : 6 * span] + picked[6 * span :]
                for v in range(2):
                    for c in range(3):
                        value = jnp.zeros((per_rep, BLOCK), jnp.float32)
                        for t in range(0, span, per_rep):
                            at = c * span + t
                            block = picked[at : at + per_rep, v * BLOCK : (v + 1) * BLOCK]
                            value = value + jnp.where(group[v] == t, block, 0.0)
                        part[first + u, 3 + c, s + v : s + v + 1, :] = jnp.sum(
                            value, axis=0, keepdims=True
                        )

    def look_up(first):
        look_up_dot(first)
        look_up_lanes(first)

    width = prod.shape[1]
    ones = jnp.ones((8, BLOCK), jnp.float32)

    def terms(k):
        p = [inbox[k, c * per_rep : (c + 1) * per_rep, :] for c in range(3)]
        q = [part[k, c] for c in range(3)]
        m = [part[k, c] for c in range(3, 6)]
        resid = m[0] * (p[0] - q[0]) + m[1] * (p[1] - q[1]) + m[2] * (p[2] - q[2])
        weight = 1.0 / (1.0 + resid * resid)
        jacob = [
            p[1] * m[2] - p[2] * m[1],
            p[2] * m[0] - p[0] * m[2],
            p[0] * m[1] - p[1] * m[0],
            m[0],
            m[1],
            m[2],
        ]
        for i in range(6):
            scaled = jacob[i] * weight
            for j in range(i, 6):
                line = jnp.sum(scaled * jacob[j], axis=0, keepdims=True)
                prod[k, 6 * i + j : 6 * i + j + 1, :] = line
                if j != i:
                    prod[k, 6 * j + i : 6 * j + i + 1, :] = line
            prod[k, 36 + i : 37 + i, :] = jnp.sum(scaled * resid, axis=0, keepdims=True)

    def finish(first):
        for u in range(2):
            terms(first + u)
        for u in range(2):
            sums = lax.dot_general(
                ones, prod[first + u], (((1,), (1,)), ((), ())),
                precision=lax.Precision.HIGHEST, preferred_element_type=jnp.float32,
            )
            res[first + u, :, :width] = sums[:1] / (reps * per_rep * BLOCK)

    def send_back(first):
        for u in range(2):
            k = first + u - 2
            for r in range(reps):
                returned(k, r).start()

    def wait_pair(first):
        incoming(first).wait_recv()

    pairs = rounds // 2
    own_pairs = n_own // 2
    turns = jnp.logical_and(me < PLANE, own_pairs == 0)

    def low_at(i):
        turned = jnp.where(i == 0, 0, jnp.where(i == pairs - 1, 1, i + 1))
        return jnp.where(turns, turned, own_pairs + i)

    def own_pair(i, carry):
        first = 2 * i + 2
        wait_pair(first)
        finish(first - 2)
        look_up(first)

        @pl.when(i == 0)
        def _():
            pl.semaphore_wait(back_go, rounds)

        @pl.when(i > 0)
        def _():
            send_back(first - 2)

        return carry

    lax.fori_loop(0, own_pairs, own_pair, 0)

    @pl.when(own_pairs > 0)
    def _():
        finish(2 * own_pairs)
        send_back(2 * own_pairs)

    @pl.when(own_pairs == 0)
    def _():
        pl.semaphore_wait(back_go, rounds)

    @pl.when(wraps)
    def _():
        for c in range(CHUNKS):
            push(c).wait_recv()
            share(c, half).start()
        pltpu.make_async_remote_copy(
            src_ref=tab.at[0, :, pl.ds(3 * partner, 3)],
            dst_ref=tab.at[1, :, pl.ds(3 * partner, 3)],
            send_sem=push_send,
            recv_sem=share_recv,
            device_id={"blk": me, "rep": partner},
            device_id_type=MESH,
        ).wait_recv()
        split_table(1)

        def low_pair(i, carry):
            before = jnp.where(i > 0, 2 * low_at(jnp.maximum(i - 1, 0)) + 2, 0)
            first = 2 * low_at(i) + 2
            wait_pair(first)
            finish(before)
            look_up(first)

            @pl.when(i > 0)
            def _():
                send_back(before)

            return carry

        lax.fori_loop(0, pairs - own_pairs, low_pair, 0)
        final = 2 * low_at(pairs - own_pairs - 1) + 2
        finish(final)
        send_back(final)

    lanes = lax.broadcasted_iota(jnp.int32, (1, BLOCK), 1)
    sign = jnp.where(lanes < 36, 1.0, -1.0)
    total = jnp.zeros((1, BLOCK), jnp.float32)
    lower = jnp.zeros((1, BLOCK), jnp.float32)
    for k in range(rounds):
        mine = k < n_own
        total = total + jnp.where(mine, res[k + 2], 0.0)
        lower = lower + jnp.where(mine, 0.0, res[k + 2])
    own[...] = total * sign
    swap = pltpu.make_async_remote_copy(
        src_ref=own,
        dst_ref=other,
        send_sem=pair_send,
        recv_sem=pair_recv,
        device_id={"blk": me, "rep": partner},
        device_id_type=MESH,
    )
    swap.start()

    @pl.when(wraps)
    def _():
        low_sum[...] = lower * sign
        pl.semaphore_wait(low_go, reps)
        for r in range(reps):
            lowered(r).start()

    pltpu.make_async_remote_copy(
        src_ref=stage,
        dst_ref=inbox.at[0:rounds],
        send_sem=out_send,
        recv_sem=out_recv.at[0],
        device_id={"blk": above, "rep": half},
        device_id_type=MESH,
    ).wait_send()

    @pl.when(wraps)
    def _():
        pltpu.make_async_remote_copy(
            src_ref=tab.at[0],
            dst_ref=tab.at[1],
            send_sem=push_send,
            recv_sem=push_recv.at[0],
            device_id={"blk": above, "rep": half},
            device_id_type=MESH,
        ).wait_send()
        raised().wait_send()

    arrivals().wait_send()
    swap.wait()
    total = own[...] + other[...]
    arrivals().wait_recv()
    for k in range(rounds):
        both = got[k, 0] + got[k, 1]
        out[k : k + 1, :] = both
        total = total + both
    own[...] = total

    @pl.when(wraps)
    def _():
        raised().wait_recv()
        own[...] = own[...] + high_sum[0] + high_sum[1]

    out[rounds : rounds + 1, :] = own[...] / (2.0 * rounds)


def split(sums, diag_ref, grad_ref, pair_ref):
    rounds = pair_ref.shape[0]
    for k in range(rounds):
        pair_ref[k, 0] = sums[k : k + 1, :36]
    diag_ref[...] = sums[rounds : rounds + 1, :36]
    grad_ref[...] = sums[rounds : rounds + 1, 36:42]


def by_rows(scan):
    return jnp.moveaxis(scan, 1, 0).reshape(scan.shape[1], -1, BLOCK)


def body(n, reps, points, normals, src_block, tgt_index, active):
    rounds, count = src_block.shape[:2]
    per_rep = src_block.shape[3]
    if count != 1 or reps != 2 or n % PLANE or n <= PLANE or rounds > PLANE // 2 or rounds % 2:
        raise ValueError("unsupported sizes")
    vmem = pl.BlockSpec(memory_space=pltpu.VMEM)
    f32, i32 = jnp.float32, jnp.int32
    rows = points.shape[2] // BLOCK
    dma = pltpu.SemaphoreType.DMA
    sums = pl.pallas_call(
        functools.partial(kernel, n, reps),
        out_shape=pltpu.VMEM((rounds + 1, BLOCK), f32),
        in_specs=[pl.BlockSpec(memory_space=pl.ANY)] * 5,
        out_specs=vmem,
        scratch_shapes=[
            pltpu.VMEM((3, rows, BLOCK), f32),
            pltpu.VMEM((2, CHUNKS, 6, rows // CHUNKS, BLOCK), f32),
            pltpu.VMEM((2, 9 * rows // CHUNKS, CHUNKS * BLOCK), f32),
            pltpu.SMEM(src_block.shape, i32),
            pltpu.VMEM(tgt_index.shape, i32),
            pltpu.SMEM((1, rounds), i32),
            pltpu.VMEM((rounds, 4 * per_rep, BLOCK), f32),
            pltpu.VMEM((rounds + 2, 4 * per_rep, BLOCK), f32),
            pltpu.VMEM((rounds + 2, 6, per_rep, BLOCK), f32),
            pltpu.VMEM((rounds + 2, 48, BLOCK), f32),
            pltpu.VMEM((rounds + 2, 1, BLOCK), f32),
            pltpu.VMEM((rounds, reps, 1, BLOCK), f32),
            pltpu.VMEM((1, BLOCK), f32),
            pltpu.VMEM((1, BLOCK), f32),
            pltpu.VMEM((1, BLOCK), f32),
            pltpu.VMEM((reps, 1, BLOCK), f32),
            dma((4,)),
            dma,
            dma,
            dma((rounds // 2,)),
            dma,
            dma,
            dma,
            dma,
            dma,
            dma((CHUNKS,)),
            dma,
            dma,
            dma,
            pltpu.SemaphoreType.REGULAR,
            pltpu.SemaphoreType.REGULAR,
        ],
        compiler_params=pltpu.CompilerParams(collective_id=0, has_side_effects=True),
        name="normal_equations",
    )(by_rows(points), by_rows(normals), src_block, tgt_index, active.reshape(1, rounds))
    return pl.pallas_call(
        split,
        out_shape=(
            jax.ShapeDtypeStruct((1, 36), f32),
            jax.ShapeDtypeStruct((1, 6), f32),
            jax.ShapeDtypeStruct((rounds, 1, 1, 36), f32),
        ),
        in_specs=[vmem],
        out_specs=(vmem, vmem, vmem),
        name="split_sums",
    )(pltpu.with_memory_space_constraint(sums, pltpu.VMEM))


def solution(mesh):
    return jax.shard_map(
        functools.partial(body, mesh.shape["blk"], mesh.shape["rep"]),
        mesh=mesh,
        in_specs=(
            P("blk", None, None),
            P("blk", None, None),
            P(None, "blk", None, "rep"),
            P(None, "blk", None, "rep", None),
            P(None, "blk", None),
        ),
        out_specs=(P("blk", None), P("blk", None), P(None, "blk", None, None)),
        check_vma=False,
    )
```

```python
import functools

import jax
import jax.numpy as jnp
from jax import lax
from jax.experimental import pallas as pl
from jax.experimental.pallas import tpu as pltpu
from jax.sharding import PartitionSpec as P

BLOCK = 128
PLANE = 16
CHUNKS = 2
GROUP = 4
MESH = pl.DeviceIdType.MESH


def kernel(
    n, reps, pts_hbm, nrm_hbm, src_hbm, tgt_hbm, act_hbm, out,
    pts, tab, cut, src, tgt, act, stage, inbox, part, prod, res, got, own, other, low_sum, high_sum,
    load, fill, out_send, out_recv, back_send, back_recv, pair_send, pair_recv,
    push_send, push_recv, share_recv, low_send, low_recv, low_go, back_go,
):
    rounds, per_rep = tgt.shape[0], tgt.shape[3]
    rows = pts.shape[1]
    span = rows // CHUNKS
    npts = rows * BLOCK
    me = lax.axis_index("blk")
    half = lax.axis_index("rep")
    partner = 1 - half
    spot = lax.rem(me, PLANE)
    base = me - spot
    above = lax.rem(me + PLANE, n)
    below = lax.rem(me + n - PLANE, n)
    wraps = spot >= PLANE - rounds
    n_own = jnp.minimum(rounds, PLANE - 1 - spot)

    def peer(d):
        return base + lax.rem(spot + d, PLANE)

    sub = lax.broadcasted_iota(jnp.int32, (per_rep, BLOCK), 0)

    def split_table(side):
        for c in range(3):
            for chunk in range(CHUNKS):
                value = tab[side, chunk, 3 + c]
                lanes = slice(chunk * BLOCK, (chunk + 1) * BLOCK)
                for piece in range(3):
                    high = value.astype(jnp.bfloat16)
                    at = (3 * piece + c) * span
                    cut[side, at : at + span, lanes] = high
                    value = value - high.astype(jnp.float32)

    barrier = pltpu.get_barrier_semaphore()
    for d in range(rounds, 0, -1):
        for r in range(reps):
            pl.semaphore_signal(
                barrier, inc=1, device_id={"blk": peer(d), "rep": r}, device_id_type=MESH
            )
    for r in range(reps):
        pl.semaphore_signal(
            barrier, inc=1, device_id={"blk": below, "rep": r}, device_id_type=MESH
        )
    pl.semaphore_signal(barrier, inc=1, device_id={"blk": me, "rep": partner}, device_id_type=MESH)

    loads = [
        pltpu.make_async_copy(a, b, load.at[i])
        for i, (a, b) in enumerate(((src_hbm, src), (act_hbm, act), (tgt_hbm, tgt), (pts_hbm, pts)))
    ]
    fills = [
        pltpu.make_async_copy(
            a.at[:, c * span : (c + 1) * span, :], tab.at[0, c, 3 * i : 3 * i + 3], fill
        )
        for c in range(CHUNKS)
        for i, a in enumerate((pts_hbm, nrm_hbm))
    ]
    for copy in loads + fills:
        copy.start()

    prod[...] = jnp.zeros_like(prod)
    res[...] = jnp.zeros_like(res)
    for copy in loads:
        copy.wait()

    slot = lax.broadcasted_iota(jnp.int32, (per_rep, BLOCK), 0) + half * per_rep
    for k in range(rounds):
        for j in range(per_rep):
            block = src[k, 0, 0, j]
            for c in range(3):
                stage[k, c * per_rep + j, :] = pts[c, block]
        index = jnp.where(slot < act[0, k], tgt[k, 0, 0], npts)
        stage[k, 3 * per_rep :, :] = index.astype(jnp.float32)
    pltpu.make_async_copy(tab.at[1], tab.at[0], fill).wait()

    split_table(0)
    pl.semaphore_wait(barrier, rounds * reps + reps + 1)

    def outgoing(k):
        return pltpu.make_async_remote_copy(
            src_ref=stage.at[k],
            dst_ref=inbox.at[k],
            send_sem=out_send,
            recv_sem=out_recv.at[k],
            device_id={"blk": peer(PLANE - 1 - k), "rep": half},
            device_id_type=MESH,
        )

    def incoming(k):
        return pltpu.make_async_remote_copy(
            src_ref=stage.at[0],
            dst_ref=inbox.at[k],
            send_sem=out_send,
            recv_sem=out_recv.at[k],
            device_id={"blk": above, "rep": half},
            device_id_type=MESH,
        )

    def returned(k, r):
        return pltpu.make_async_remote_copy(
            src_ref=res.at[k],
            dst_ref=got.at[k, half],
            send_sem=back_send,
            recv_sem=back_recv,
            device_id={"blk": peer(k + 1), "rep": r},
            device_id_type=MESH,
        )

    def arrivals():
        return pltpu.make_async_remote_copy(
            src_ref=got,
            dst_ref=got,
            send_sem=back_send,
            recv_sem=back_recv,
            device_id={"blk": above, "rep": half},
            device_id_type=MESH,
        )

    def push(c):
        return pltpu.make_async_remote_copy(
            src_ref=tab.at[0, c, pl.ds(3 * half, 3)],
            dst_ref=tab.at[1, c, pl.ds(3 * half, 3)],
            send_sem=push_send,
            recv_sem=push_recv.at[c],
            device_id={"blk": above, "rep": half},
            device_id_type=MESH,
        )

    def share(c, at):
        return pltpu.make_async_remote_copy(
            src_ref=tab.at[1, c, pl.ds(3 * at, 3)],
            dst_ref=tab.at[1, c, pl.ds(3 * at, 3)],
            send_sem=push_send,
            recv_sem=share_recv,
            device_id={"blk": me, "rep": partner},
            device_id_type=MESH,
        )

    def lowered(r):
        return pltpu.make_async_remote_copy(
            src_ref=low_sum,
            dst_ref=high_sum.at[half],
            send_sem=low_send,
            recv_sem=low_recv,
            device_id={"blk": below, "rep": r},
            device_id_type=MESH,
        )

    def raised():
        return pltpu.make_async_remote_copy(
            src_ref=high_sum,
            dst_ref=high_sum,
            send_sem=low_send,
            recv_sem=low_recv,
            device_id={"blk": below, "rep": half},
            device_id_type=MESH,
        )

    @pl.when(wraps)
    def _():
        for c in range(CHUNKS):
            push(c).start()

    for k in range(rounds):
        outgoing(k).start()
    for k in range(rounds):
        pl.semaphore_signal(
            back_go, inc=1,
            device_id={"blk": peer(PLANE - 1 - k), "rep": partner}, device_id_type=MESH,
        )

    @pl.when(wraps)
    def _():
        for r in range(reps):
            pl.semaphore_signal(
                low_go, inc=1, device_id={"blk": above, "rep": r}, device_id_type=MESH
            )

    def points_of(k, side):
        index = inbox[k, 3 * per_rep :, :].astype(jnp.int32)
        lane = index & (BLOCK - 1)
        row = index >> (BLOCK.bit_length() - 1)
        found = [jnp.zeros((per_rep, BLOCK), jnp.float32) for c in range(3)]
        for chunk in range(CHUNKS):
            for h in range(span):
                here = row == chunk * span + h
                for c in range(3):
                    line = jnp.broadcast_to(tab[side, chunk, c, h : h + 1, :], (per_rep, BLOCK))
                    value = jnp.take_along_axis(line, lane, axis=1, mode="promise_in_bounds")
                    found[c] = jnp.where(here, value, found[c])
        return found

    def look_up_normals(k, side):
        for s in range(0, per_rep, 2):
            hot, group = [], []
            for v in range(2):
                at = 3 * per_rep + s + v
                line = jnp.broadcast_to(inbox[k, at : at + 1, :], (per_rep, BLOCK))
                line = line.astype(jnp.int32)
                row = line >> (BLOCK.bit_length() - 1)
                column = (line & (BLOCK - 1)) + (row >> (span.bit_length() - 1)) * BLOCK - sub
                group.append((row & (span - 1)) - sub)
                hot.append(jnp.concatenate([
                    jnp.where(column == i, 1.0, 0.0) for i in range(0, CHUNKS * BLOCK, per_rep)
                ], axis=0))
            picked = lax.dot_general(
                cut[side], jnp.concatenate(hot, axis=1).astype(jnp.bfloat16),
                (((1,), (0,)), ((), ())), preferred_element_type=jnp.float32,
            )
            picked = picked[: 3 * span] + picked[3 * span : 6 * span] + picked[6 * span :]
            for v in range(2):
                for c in range(3):
                    value = jnp.zeros((per_rep, BLOCK), jnp.float32)
                    for t in range(0, span, per_rep):
                        at = c * span + t
                        block = picked[at : at + per_rep, v * BLOCK : (v + 1) * BLOCK]
                        value = value + jnp.where(group[v] == t, block, 0.0)
                    part[k, c, s + v : s + v + 1, :] = jnp.sum(value, axis=0, keepdims=True)

    width = prod.shape[1]
    ones = jnp.ones((8, BLOCK), jnp.float32)

    def terms(k, q):
        p = [inbox[k, c * per_rep : (c + 1) * per_rep, :] for c in range(3)]
        m = [part[k, c] for c in range(3)]
        resid = m[0] * (p[0] - q[0]) + m[1] * (p[1] - q[1]) + m[2] * (p[2] - q[2])
        weight = 1.0 / (1.0 + resid * resid)
        jacob = [
            p[1] * m[2] - p[2] * m[1],
            p[2] * m[0] - p[0] * m[2],
            p[0] * m[1] - p[1] * m[0],
            m[0],
            m[1],
            m[2],
        ]
        for i in range(6):
            scaled = jacob[i] * weight
            for j in range(i, 6):
                line = jnp.sum(scaled * jacob[j], axis=0, keepdims=True)
                prod[k, 6 * i + j : 6 * i + j + 1, :] = line
                if j != i:
                    prod[k, 6 * j + i : 6 * j + i + 1, :] = line
            prod[k, 36 + i : 37 + i, :] = jnp.sum(scaled * resid, axis=0, keepdims=True)

    own_groups = n_own // GROUP
    groups = rounds // GROUP
    turns = jnp.logical_and(me < PLANE, own_groups == 0)
    early = PLANE - 1 - spot

    def work(ks):
        for k in ks:
            incoming(k).wait_recv()
        for k in ks:
            side = jnp.where(k < n_own, 0, 1)
            look_up_normals(k, side)
            terms(k, points_of(k, side))
        for k in ks:
            sums = lax.dot_general(
                ones, prod[k], (((1,), (1,)), ((), ())),
                precision=lax.Precision.HIGHEST, preferred_element_type=jnp.float32,
            )
            res[k, :, :width] = sums[:1] / (reps * per_rep * BLOCK)
        for k in ks:
            for r in range(reps):
                returned(k, r).start()

    def plain(g, carry):
        work([GROUP * g + u for u in range(GROUP)])
        return carry

    pl.semaphore_wait(back_go, rounds)
    lax.fori_loop(0, own_groups, plain, 0)

    @pl.when(wraps)
    def _():
        for c in range(CHUNKS):
            push(c).wait_recv()
            share(c, half).start()
        pltpu.make_async_remote_copy(
            src_ref=tab.at[0, :, pl.ds(3 * partner, 3)],
            dst_ref=tab.at[1, :, pl.ds(3 * partner, 3)],
            send_sem=push_send,
            recv_sem=share_recv,
            device_id={"blk": me, "rep": partner},
            device_id_type=MESH,
        ).wait_recv()
        split_table(1)

        @pl.when(turns)
        def _():
            others = [u + jnp.where(u >= early, 1, 0) for u in range(GROUP - 1)]
            work([early, GROUP + 1])
            work([GROUP, GROUP + 2, GROUP + 3] + others)

        @pl.when(jnp.logical_not(turns))
        def _():
            lax.fori_loop(own_groups, groups, plain, 0)

    lanes = lax.broadcasted_iota(jnp.int32, (1, BLOCK), 1)
    sign = jnp.where(lanes < 36, 1.0, -1.0)
    total = jnp.zeros((1, BLOCK), jnp.float32)
    lower = jnp.zeros((1, BLOCK), jnp.float32)
    for k in range(rounds):
        mine = k < n_own
        total = total + jnp.where(mine, res[k], 0.0)
        lower = lower + jnp.where(mine, 0.0, res[k])
    own[...] = total * sign
    swap = pltpu.make_async_remote_copy(
        src_ref=own,
        dst_ref=other,
        send_sem=pair_send,
        recv_sem=pair_recv,
        device_id={"blk": me, "rep": partner},
        device_id_type=MESH,
    )
    swap.start()

    @pl.when(wraps)
    def _():
        low_sum[...] = lower * sign
        pl.semaphore_wait(low_go, reps)
        for r in range(reps):
            lowered(r).start()

    pltpu.make_async_remote_copy(
        src_ref=stage,
        dst_ref=inbox,
        send_sem=out_send,
        recv_sem=out_recv.at[0],
        device_id={"blk": above, "rep": half},
        device_id_type=MESH,
    ).wait_send()

    @pl.when(wraps)
    def _():
        pltpu.make_async_remote_copy(
            src_ref=tab.at[0],
            dst_ref=tab.at[1],
            send_sem=push_send,
            recv_sem=push_recv.at[0],
            device_id={"blk": above, "rep": half},
            device_id_type=MESH,
        ).wait_send()
        raised().wait_send()

    arrivals().wait_send()
    swap.wait()
    total = own[...] + other[...]
    arrivals().wait_recv()
    for k in range(rounds):
        both = got[k, 0] + got[k, 1]
        out[k : k + 1, :] = both
        total = total + both
    own[...] = total

    @pl.when(wraps)
    def _():
        raised().wait_recv()
        own[...] = own[...] + high_sum[0] + high_sum[1]

    out[rounds : rounds + 1, :] = own[...] / (2.0 * rounds)


def split(sums, diag_ref, grad_ref, pair_ref):
    rounds = pair_ref.shape[0]
    for k in range(rounds):
        pair_ref[k, 0] = sums[k : k + 1, :36]
    diag_ref[...] = sums[rounds : rounds + 1, :36]
    grad_ref[...] = sums[rounds : rounds + 1, 36:42]


def by_rows(scan):
    return jnp.moveaxis(scan, 1, 0).reshape(scan.shape[1], -1, BLOCK)


def body(n, reps, points, normals, src_block, tgt_index, active):
    rounds, count = src_block.shape[:2]
    per_rep = src_block.shape[3]
    if count != 1 or reps != 2 or n % PLANE or n <= PLANE or rounds > PLANE // 2 or rounds != 2 * GROUP:
        raise ValueError("unsupported sizes")
    vmem = pl.BlockSpec(memory_space=pltpu.VMEM)
    f32, i32 = jnp.float32, jnp.int32
    rows = points.shape[2] // BLOCK
    dma = pltpu.SemaphoreType.DMA
    sums = pl.pallas_call(
        functools.partial(kernel, n, reps),
        out_shape=pltpu.VMEM((rounds + 1, BLOCK), f32),
        in_specs=[pl.BlockSpec(memory_space=pl.ANY)] * 5,
        out_specs=vmem,
        scratch_shapes=[
            pltpu.VMEM((3, rows, BLOCK), f32),
            pltpu.VMEM((2, CHUNKS, 6, rows // CHUNKS, BLOCK), f32),
            pltpu.VMEM((2, 9 * rows // CHUNKS, CHUNKS * BLOCK), jnp.bfloat16),
            pltpu.SMEM(src_block.shape, i32),
            pltpu.VMEM(tgt_index.shape, i32),
            pltpu.SMEM((1, rounds), i32),
            pltpu.VMEM((rounds, 4 * per_rep, BLOCK), f32),
            pltpu.VMEM((rounds, 4 * per_rep, BLOCK), f32),
            pltpu.VMEM((rounds, 3, per_rep, BLOCK), f32),
            pltpu.VMEM((rounds, 48, BLOCK), f32),
            pltpu.VMEM((rounds, 1, BLOCK), f32),
            pltpu.VMEM((rounds, reps, 1, BLOCK), f32),
            pltpu.VMEM((1, BLOCK), f32),
            pltpu.VMEM((1, BLOCK), f32),
            pltpu.VMEM((1, BLOCK), f32),
            pltpu.VMEM((reps, 1, BLOCK), f32),
            dma((4,)),
            dma,
            dma,
            dma((rounds,)),
            dma,
            dma,
            dma,
            dma,
            dma,
            dma((CHUNKS,)),
            dma,
            dma,
            dma,
            pltpu.SemaphoreType.REGULAR,
            pltpu.SemaphoreType.REGULAR,
        ],
        compiler_params=pltpu.CompilerParams(collective_id=0, has_side_effects=True),
        name="normal_equations",
    )(by_rows(points), by_rows(normals), src_block, tgt_index, active.reshape(1, rounds))
    return pl.pallas_call(
        split,
        out_shape=(
            jax.ShapeDtypeStruct((1, 36), f32),
            jax.ShapeDtypeStruct((1, 6), f32),
            jax.ShapeDtypeStruct((rounds, 1, 1, 36), f32),
        ),
        in_specs=[vmem],
        out_specs=(vmem, vmem, vmem),
        name="split_sums",
    )(pltpu.with_memory_space_constraint(sums, pltpu.VMEM))


def solution(mesh):
    return jax.shard_map(
        functools.partial(body, mesh.shape["blk"], mesh.shape["rep"]),
        mesh=mesh,
        in_specs=(
            P("blk", None, None),
            P("blk", None, None),
            P(None, "blk", None, "rep"),
            P(None, "blk", None, "rep", None),
            P(None, "blk", None),
        ),
        out_specs=(P("blk", None), P("blk", None), P(None, "blk", None, None)),
        check_vma=False,
    )
```

```python
import functools

import jax
import jax.numpy as jnp
from jax import lax
from jax.experimental import pallas as pl
from jax.experimental.pallas import tpu as pltpu
from jax.sharding import PartitionSpec as P

BLOCK = 128
PLANE = 16
CHUNKS = 2
GROUP = 4
MESH = pl.DeviceIdType.MESH


def kernel(
    n, reps, pts_hbm, nrm_hbm, src_hbm, tgt_hbm, act_hbm, out,
    pts, tab, cut, src, tgt, act, stage, inbox, part, prod, res, got, own, other, low_sum, high_sum,
    load, fill, out_send, out_recv, back_send, back_recv, pair_send, pair_recv,
    push_send, push_recv, low_send, low_recv,
):
    rounds, per_rep = tgt.shape[0], tgt.shape[3]
    rows = pts.shape[1]
    span = rows // CHUNKS
    npts = rows * BLOCK
    me = lax.axis_index("blk")
    half = lax.axis_index("rep")
    partner = 1 - half
    spot = lax.rem(me, PLANE)
    base = me - spot
    above = lax.rem(me + PLANE, n)
    below = lax.rem(me + n - PLANE, n)
    wraps = spot >= PLANE - rounds
    lead = half == reps - 1
    n_own = jnp.minimum(rounds, PLANE - 1 - spot)

    def peer(d):
        return base + lax.rem(spot + d, PLANE)

    sub = lax.broadcasted_iota(jnp.int32, (per_rep, BLOCK), 0)

    def split_table(side):
        for c in range(3):
            for chunk in range(CHUNKS):
                value = tab[side, chunk, 3 + c]
                lanes = slice(chunk * BLOCK, (chunk + 1) * BLOCK)
                for piece in range(3):
                    high = value.astype(jnp.bfloat16)
                    at = (3 * piece + c) * span
                    cut[side, at : at + span, lanes] = high
                    value = value - high.astype(jnp.float32)

    barrier = pltpu.get_barrier_semaphore()
    for d in (6, 7, 2, 5, 8, 3, 1, 4):
        pl.semaphore_signal(
            barrier, inc=1, device_id={"blk": peer(d), "rep": half}, device_id_type=MESH
        )
    pl.semaphore_signal(barrier, inc=1, device_id={"blk": me, "rep": partner}, device_id_type=MESH)
    pl.semaphore_signal(barrier, inc=1, device_id={"blk": below, "rep": half}, device_id_type=MESH)

    loads = [
        pltpu.make_async_copy(a, b, load.at[i])
        for i, (a, b) in enumerate(((src_hbm, src), (act_hbm, act), (tgt_hbm, tgt), (pts_hbm, pts)))
    ]
    fills = [
        pltpu.make_async_copy(
            a.at[:, c * span : (c + 1) * span, :], tab.at[0, c, 3 * i : 3 * i + 3], fill
        )
        for c in range(CHUNKS)
        for i, a in enumerate((pts_hbm, nrm_hbm))
    ]
    for copy in loads + fills:
        copy.start()

    prod[...] = jnp.zeros_like(prod)
    res[...] = jnp.zeros_like(res)
    for copy in loads:
        copy.wait()

    slot = lax.broadcasted_iota(jnp.int32, (per_rep, BLOCK), 0) + half * per_rep
    for k in range(rounds):
        for j in range(per_rep):
            block = src[k, 0, 0, j]
            for c in range(3):
                stage[k, c * per_rep + j, :] = pts[c, block]
        index = jnp.where(slot < act[0, k], tgt[k, 0, 0], npts)
        stage[k, 3 * per_rep :, :] = index.astype(jnp.float32)
    pltpu.make_async_copy(tab.at[1], tab.at[0], fill).wait()

    split_table(0)
    pl.semaphore_wait(barrier, rounds + 2)

    def outgoing(k):
        return pltpu.make_async_remote_copy(
            src_ref=stage.at[k],
            dst_ref=inbox.at[k],
            send_sem=out_send,
            recv_sem=out_recv.at[k],
            device_id={"blk": peer(PLANE - 1 - k), "rep": half},
            device_id_type=MESH,
        )

    def incoming(k):
        return pltpu.make_async_remote_copy(
            src_ref=stage.at[0],
            dst_ref=inbox.at[k],
            send_sem=out_send,
            recv_sem=out_recv.at[k],
            device_id={"blk": above, "rep": half},
            device_id_type=MESH,
        )

    def returned(k, r):
        return pltpu.make_async_remote_copy(
            src_ref=res.at[k],
            dst_ref=got.at[k, half],
            send_sem=back_send,
            recv_sem=back_recv,
            device_id={"blk": peer(k + 1), "rep": r},
            device_id_type=MESH,
        )

    def arrivals():
        return pltpu.make_async_remote_copy(
            src_ref=got,
            dst_ref=got,
            send_sem=back_send,
            recv_sem=back_recv,
            device_id={"blk": above, "rep": half},
            device_id_type=MESH,
        )

    def piece(side, i):
        return tab.at[side, i // 2, 3 * (i % 2) : 3 * (i % 2) + 3]

    def push(i):
        return pltpu.make_async_remote_copy(
            src_ref=piece(0, i),
            dst_ref=piece(1, i),
            send_sem=push_send,
            recv_sem=push_recv.at[i],
            device_id={"blk": above, "rep": half},
            device_id_type=MESH,
        )

    def share(i):
        return pltpu.make_async_remote_copy(
            src_ref=piece(1, i),
            dst_ref=piece(1, i),
            send_sem=push_send,
            recv_sem=push_recv.at[i],
            device_id={"blk": me, "rep": partner},
            device_id_type=MESH,
        )

    def lowered(r):
        return pltpu.make_async_remote_copy(
            src_ref=low_sum,
            dst_ref=high_sum.at[half],
            send_sem=low_send,
            recv_sem=low_recv,
            device_id={"blk": below, "rep": r},
            device_id_type=MESH,
        )

    def raised():
        return pltpu.make_async_remote_copy(
            src_ref=high_sum,
            dst_ref=high_sum,
            send_sem=low_send,
            recv_sem=low_recv,
            device_id={"blk": below, "rep": half},
            device_id_type=MESH,
        )

    @pl.when(jnp.logical_and(wraps, lead))
    def _():
        for i in range(2 * CHUNKS):
            push(i).start()

    for k in range(rounds):
        outgoing(k).start()
    def points_of(k, side):
        index = inbox[k, 3 * per_rep :, :].astype(jnp.int32)
        lane = index & (BLOCK - 1)
        row = index >> (BLOCK.bit_length() - 1)
        found = [jnp.zeros((per_rep, BLOCK), jnp.float32) for c in range(3)]
        for chunk in range(CHUNKS):
            for h in range(span):
                here = row == chunk * span + h
                for c in range(3):
                    line = jnp.broadcast_to(tab[side, chunk, c, h : h + 1, :], (per_rep, BLOCK))
                    value = jnp.take_along_axis(line, lane, axis=1, mode="promise_in_bounds")
                    found[c] = jnp.where(here, value, found[c])
        return found

    def look_up_normals(k, side):
        for s in range(0, per_rep, 2):
            hot, group = [], []
            for v in range(2):
                at = 3 * per_rep + s + v
                line = jnp.broadcast_to(inbox[k, at : at + 1, :], (per_rep, BLOCK))
                line = line.astype(jnp.int32)
                row = line >> (BLOCK.bit_length() - 1)
                column = (line & (BLOCK - 1)) + (row >> (span.bit_length() - 1)) * BLOCK - sub
                group.append((row & (span - 1)) - sub)
                hot.append(jnp.concatenate([
                    jnp.where(column == i, 1.0, 0.0) for i in range(0, CHUNKS * BLOCK, per_rep)
                ], axis=0))
            picked = lax.dot_general(
                cut[side], jnp.concatenate(hot, axis=1).astype(jnp.bfloat16),
                (((1,), (0,)), ((), ())), preferred_element_type=jnp.float32,
            )
            picked = picked[: 3 * span] + picked[3 * span : 6 * span] + picked[6 * span :]
            for v in range(2):
                for c in range(3):
                    value = jnp.zeros((per_rep, BLOCK), jnp.float32)
                    for t in range(0, span, per_rep):
                        at = c * span + t
                        block = picked[at : at + per_rep, v * BLOCK : (v + 1) * BLOCK]
                        value = value + jnp.where(group[v] == t, block, 0.0)
                    part[k, c, s + v : s + v + 1, :] = jnp.sum(value, axis=0, keepdims=True)

    width = prod.shape[1]
    ones = jnp.ones((8, BLOCK), jnp.float32)

    def terms(k, q):
        p = [inbox[k, c * per_rep : (c + 1) * per_rep, :] for c in range(3)]
        m = [part[k, c] for c in range(3)]
        resid = m[0] * (p[0] - q[0]) + m[1] * (p[1] - q[1]) + m[2] * (p[2] - q[2])
        weight = 1.0 / (1.0 + resid * resid)
        jacob = [
            p[1] * m[2] - p[2] * m[1],
            p[2] * m[0] - p[0] * m[2],
            p[0] * m[1] - p[1] * m[0],
            m[0],
            m[1],
            m[2],
        ]
        for i in range(6):
            scaled = jacob[i] * weight
            for j in range(i, 6):
                line = jnp.sum(scaled * jacob[j], axis=0, keepdims=True)
                prod[k, 6 * i + j : 6 * i + j + 1, :] = line
                if j != i:
                    prod[k, 6 * j + i : 6 * j + i + 1, :] = line
            prod[k, 36 + i : 37 + i, :] = jnp.sum(scaled * resid, axis=0, keepdims=True)

    own_groups = n_own // GROUP
    groups = rounds // GROUP
    turns = jnp.logical_and(me < PLANE, own_groups == 0)
    early = PLANE - 1 - spot

    def work(ks):
        for k in ks:
            incoming(k).wait_recv()
        for k in ks:
            side = jnp.where(k < n_own, 0, 1)
            look_up_normals(k, side)
            terms(k, points_of(k, side))
        for k in ks:
            sums = lax.dot_general(
                ones, prod[k], (((1,), (1,)), ((), ())),
                precision=lax.Precision.HIGHEST, preferred_element_type=jnp.float32,
            )
            res[k, :, :width] = sums[:1] / (reps * per_rep * BLOCK)
        for k in ks:
            for r in range(reps):
                returned(k, r).start()

    deep = jnp.logical_and(turns, early >= 2)

    @pl.when(deep)
    def _():
        work([0, 1])

    def plain(g, carry):
        work([GROUP * g + u for u in range(GROUP)])
        return carry

    lax.fori_loop(0, own_groups, plain, 0)

    @pl.when(wraps)
    def _():
        for i in range(2 * CHUNKS):
            push(i).wait_recv()

            @pl.when(lead)
            def _():
                share(i).start()

        split_table(1)

        @pl.when(turns)
        def _():
            others = [u + jnp.where(u >= early, 1, 0) for u in range(GROUP - 1)]

            @pl.when(deep)
            def _():
                work([early, GROUP + 1])
                work([GROUP, GROUP + 2, GROUP + 3, GROUP + 1 - early])

            @pl.when(jnp.logical_not(deep))
            def _():
                work([early, GROUP + 1])
                work([GROUP, GROUP + 2, GROUP + 3] + others)

        @pl.when(jnp.logical_not(turns))
        def _():
            lax.fori_loop(own_groups, groups, plain, 0)

    lanes = lax.broadcasted_iota(jnp.int32, (1, BLOCK), 1)
    sign = jnp.where(lanes < 36, 1.0, -1.0)
    total = jnp.zeros((1, BLOCK), jnp.float32)
    lower = jnp.zeros((1, BLOCK), jnp.float32)
    for k in range(rounds):
        mine = k < n_own
        total = total + jnp.where(mine, res[k], 0.0)
        lower = lower + jnp.where(mine, 0.0, res[k])
    own[...] = total * sign
    swap = pltpu.make_async_remote_copy(
        src_ref=own,
        dst_ref=other,
        send_sem=pair_send,
        recv_sem=pair_recv,
        device_id={"blk": me, "rep": partner},
        device_id_type=MESH,
    )
    swap.start()

    @pl.when(wraps)
    def _():
        low_sum[...] = lower * sign
        for r in range(reps):
            lowered(r).start()

    pltpu.make_async_remote_copy(
        src_ref=stage,
        dst_ref=inbox,
        send_sem=out_send,
        recv_sem=out_recv.at[0],
        device_id={"blk": above, "rep": half},
        device_id_type=MESH,
    ).wait_send()

    @pl.when(jnp.logical_and(wraps, lead))
    def _():
        pltpu.make_async_remote_copy(
            src_ref=tab,
            dst_ref=tab,
            send_sem=push_send,
            recv_sem=push_recv.at[0],
            device_id={"blk": above, "rep": half},
            device_id_type=MESH,
        ).wait_send()

    @pl.when(wraps)
    def _():
        raised().wait_send()

    arrivals().wait_send()
    swap.wait()
    total = own[...] + other[...]
    arrivals().wait_recv()
    for k in range(rounds):
        both = got[k, 0] + got[k, 1]
        out[k : k + 1, :] = both
        total = total + both
    own[...] = total

    @pl.when(wraps)
    def _():
        raised().wait_recv()
        own[...] = own[...] + high_sum[0] + high_sum[1]

    out[rounds : rounds + 1, :] = own[...] / (2.0 * rounds)


def split(sums, diag_ref, grad_ref, pair_ref):
    rounds = pair_ref.shape[0]
    for k in range(rounds):
        pair_ref[k, 0] = sums[k : k + 1, :36]
    diag_ref[...] = sums[rounds : rounds + 1, :36]
    grad_ref[...] = sums[rounds : rounds + 1, 36:42]


def by_rows(scan):
    return jnp.moveaxis(scan, 1, 0).reshape(scan.shape[1], -1, BLOCK)


def body(n, reps, points, normals, src_block, tgt_index, active):
    rounds, count = src_block.shape[:2]
    per_rep = src_block.shape[3]
    if count != 1 or reps != 2 or n % PLANE or n <= PLANE or rounds > PLANE // 2 or rounds != 2 * GROUP:
        raise ValueError("unsupported sizes")
    vmem = pl.BlockSpec(memory_space=pltpu.VMEM)
    f32, i32 = jnp.float32, jnp.int32
    rows = points.shape[2] // BLOCK
    dma = pltpu.SemaphoreType.DMA
    sums = pl.pallas_call(
        functools.partial(kernel, n, reps),
        out_shape=pltpu.VMEM((rounds + 1, BLOCK), f32),
        in_specs=[pl.BlockSpec(memory_space=pl.ANY)] * 5,
        out_specs=vmem,
        scratch_shapes=[
            pltpu.VMEM((3, rows, BLOCK), f32),
            pltpu.VMEM((2, CHUNKS, 6, rows // CHUNKS, BLOCK), f32),
            pltpu.VMEM((2, 9 * rows // CHUNKS, CHUNKS * BLOCK), jnp.bfloat16),
            pltpu.SMEM(src_block.shape, i32),
            pltpu.VMEM(tgt_index.shape, i32),
            pltpu.SMEM((1, rounds), i32),
            pltpu.VMEM((rounds, 4 * per_rep, BLOCK), f32),
            pltpu.VMEM((rounds, 4 * per_rep, BLOCK), f32),
            pltpu.VMEM((rounds, 3, per_rep, BLOCK), f32),
            pltpu.VMEM((rounds, 48, BLOCK), f32),
            pltpu.VMEM((rounds, 1, BLOCK), f32),
            pltpu.VMEM((rounds, reps, 1, BLOCK), f32),
            pltpu.VMEM((1, BLOCK), f32),
            pltpu.VMEM((1, BLOCK), f32),
            pltpu.VMEM((1, BLOCK), f32),
            pltpu.VMEM((reps, 1, BLOCK), f32),
            dma((4,)),
            dma,
            dma,
            dma((rounds,)),
            dma,
            dma,
            dma,
            dma,
            dma,
            dma((2 * CHUNKS,)),
            dma,
            dma,
        ],
        compiler_params=pltpu.CompilerParams(collective_id=0, has_side_effects=True),
        name="normal_equations",
    )(by_rows(points), by_rows(normals), src_block, tgt_index, active.reshape(1, rounds))
    return pl.pallas_call(
        split,
        out_shape=(
            jax.ShapeDtypeStruct((1, 36), f32),
            jax.ShapeDtypeStruct((1, 6), f32),
            jax.ShapeDtypeStruct((rounds, 1, 1, 36), f32),
        ),
        in_specs=[vmem],
        out_specs=(vmem, vmem, vmem),
        name="split_sums",
    )(pltpu.with_memory_space_constraint(sums, pltpu.VMEM))


def solution(mesh):
    return jax.shard_map(
        functools.partial(body, mesh.shape["blk"], mesh.shape["rep"]),
        mesh=mesh,
        in_specs=(
            P("blk", None, None),
            P("blk", None, None),
            P(None, "blk", None, "rep"),
            P(None, "blk", None, "rep", None),
            P(None, "blk", None),
        ),
        out_specs=(P("blk", None), P("blk", None), P(None, "blk", None, None)),
        check_vma=False,
    )
```

```python
import functools

import jax
import jax.numpy as jnp
from jax import lax
from jax.experimental import pallas as pl
from jax.experimental.pallas import tpu as pltpu
from jax.sharding import PartitionSpec as P

BLOCK = 128
PLANE = 16
CHUNKS = 2
GROUP = 4
MESH = pl.DeviceIdType.MESH


def kernel(
    n, reps, pts_hbm, nrm_hbm, src_hbm, tgt_hbm, act_hbm, out,
    pts, tab, cut, src, tgt, act, stage, inbox, part, seen, prod, res, got, own, other, low_sum, high_sum,
    load, fill, out_send, out_recv, back_send, back_recv, pair_send, pair_recv,
    push_send, push_recv, low_send, low_recv,
):
    rounds, per_rep = tgt.shape[0], tgt.shape[3]
    rows = pts.shape[1]
    span = rows // CHUNKS
    npts = rows * BLOCK
    me = lax.axis_index("blk")
    half = lax.axis_index("rep")
    partner = 1 - half
    spot = lax.rem(me, PLANE)
    above = me + PLANE - jnp.where(me >= n - PLANE, n, 0)
    below = me - PLANE + jnp.where(me < PLANE, n, 0)
    wraps = spot >= PLANE - rounds
    lead = half == reps - 1
    n_own = jnp.minimum(rounds, PLANE - 1 - spot)

    def peer(d):
        return me + d - jnp.where(spot + d >= PLANE, PLANE, 0)

    sub = lax.broadcasted_iota(jnp.int32, (per_rep, BLOCK), 0)

    def split_table(side):
        for c in range(3):
            for chunk in range(CHUNKS):
                value = tab[side, chunk, 3 + c]
                lanes = slice(chunk * BLOCK, (chunk + 1) * BLOCK)
                for piece in range(3):
                    high = value.astype(jnp.bfloat16)
                    at = (3 * piece + c) * span
                    cut[side, at : at + span, lanes] = high
                    value = value - high.astype(jnp.float32)

    loads = [
        pltpu.make_async_copy(a, b, load.at[i])
        for i, (a, b) in enumerate(((src_hbm, src), (act_hbm, act), (tgt_hbm, tgt), (pts_hbm, pts)))
    ]
    fills = [
        pltpu.make_async_copy(
            a.at[:, c * span : (c + 1) * span, :], tab.at[0, c, 3 * i : 3 * i + 3], fill
        )
        for c in range(CHUNKS)
        for i, a in enumerate((pts_hbm, nrm_hbm))
    ]
    barrier = pltpu.get_barrier_semaphore()
    for d in (6, 7, 2, 5, 8, 3, 1, 4):
        pl.semaphore_signal(
            barrier, inc=1, device_id={"blk": peer(d), "rep": half}, device_id_type=MESH
        )
    pl.semaphore_signal(barrier, inc=1, device_id={"blk": me, "rep": partner}, device_id_type=MESH)
    pl.semaphore_signal(
        barrier, inc=1, device_id={"blk": below, "rep": reps - 1}, device_id_type=MESH
    )

    for copy in fills + loads:
        copy.start()

    prod[...] = jnp.zeros_like(prod)
    res[...] = jnp.zeros_like(res)
    pltpu.make_async_copy(tab.at[1], tab.at[0], fill).wait()

    pl.semaphore_wait(barrier, rounds + 1 + jnp.where(lead, reps, 0))

    def outgoing(k):
        return pltpu.make_async_remote_copy(
            src_ref=stage.at[k],
            dst_ref=inbox.at[k],
            send_sem=out_send,
            recv_sem=out_recv.at[k],
            device_id={"blk": peer(PLANE - 1 - k), "rep": half},
            device_id_type=MESH,
        )

    def incoming(k):
        return pltpu.make_async_remote_copy(
            src_ref=stage.at[0],
            dst_ref=inbox.at[k],
            send_sem=out_send,
            recv_sem=out_recv.at[k],
            device_id={"blk": above, "rep": half},
            device_id_type=MESH,
        )

    def returned(k, r):
        return pltpu.make_async_remote_copy(
            src_ref=res.at[k],
            dst_ref=got.at[k, half],
            send_sem=back_send,
            recv_sem=back_recv,
            device_id={"blk": peer(k + 1), "rep": r},
            device_id_type=MESH,
        )

    def arrivals():
        return pltpu.make_async_remote_copy(
            src_ref=got,
            dst_ref=got,
            send_sem=back_send,
            recv_sem=back_recv,
            device_id={"blk": above, "rep": half},
            device_id_type=MESH,
        )

    def piece(side, i):
        at = 3 * (i // CHUNKS)
        return tab.at[side, i % CHUNKS, at : at + 3]

    final = 2 * CHUNKS - 1

    def push(i, r=reps - 1):
        return pltpu.make_async_remote_copy(
            src_ref=piece(0, i),
            dst_ref=piece(1, i),
            send_sem=push_send,
            recv_sem=push_recv.at[i],
            device_id={"blk": above, "rep": r},
            device_id_type=MESH,
        )

    def share(i):
        return pltpu.make_async_remote_copy(
            src_ref=piece(1, i),
            dst_ref=piece(1, i),
            send_sem=push_send,
            recv_sem=push_recv.at[i],
            device_id={"blk": me, "rep": partner},
            device_id_type=MESH,
        )

    def lowered(r):
        return pltpu.make_async_remote_copy(
            src_ref=low_sum,
            dst_ref=high_sum.at[half],
            send_sem=low_send,
            recv_sem=low_recv,
            device_id={"blk": below, "rep": r},
            device_id_type=MESH,
        )

    def raised():
        return pltpu.make_async_remote_copy(
            src_ref=high_sum,
            dst_ref=high_sum,
            send_sem=low_send,
            recv_sem=low_recv,
            device_id={"blk": below, "rep": half},
            device_id_type=MESH,
        )

    @pl.when(jnp.logical_and(wraps, lead))
    def _():
        for i in range(final):
            push(i).start()
        for r in range(reps):
            push(final, r).start()

    for copy in loads:
        copy.wait()

    slot = lax.broadcasted_iota(jnp.int32, (per_rep, BLOCK), 0) + half * per_rep
    for k in range(rounds):
        for j in range(per_rep):
            block = src[k, 0, 0, j]
            for c in range(3):
                stage[k, c * per_rep + j, :] = pts[c, block]
        index = jnp.where(slot < act[0, k], tgt[k, 0, 0], npts)
        stage[k, 3 * per_rep :, :] = index.astype(jnp.float32)
    for k in range(rounds):
        outgoing(k).start()
    split_table(0)
    def points_of(k, side):
        index = inbox[k, 3 * per_rep :, :].astype(jnp.int32)
        lane = index & (BLOCK - 1)
        row = index >> (BLOCK.bit_length() - 1)
        found = [jnp.zeros((per_rep, BLOCK), jnp.float32) for c in range(3)]
        for chunk in range(CHUNKS):
            for h in range(span):
                here = row == chunk * span + h
                for c in range(3):
                    line = jnp.broadcast_to(tab[side, chunk, c, h : h + 1, :], (per_rep, BLOCK))
                    value = jnp.take_along_axis(line, lane, axis=1, mode="promise_in_bounds")
                    found[c] = jnp.where(here, value, found[c])
        return found

    def look_up_normals(k, side):
        for s in range(0, per_rep, 2):
            hot, group = [], []
            for v in range(2):
                at = 3 * per_rep + s + v
                line = jnp.broadcast_to(inbox[k, at : at + 1, :], (per_rep, BLOCK))
                line = line.astype(jnp.int32)
                row = line >> (BLOCK.bit_length() - 1)
                column = (line & (BLOCK - 1)) + (row >> (span.bit_length() - 1)) * BLOCK - sub
                group.append((row & (span - 1)) - sub)
                hot.append(jnp.concatenate([
                    jnp.where(column == i, 1.0, 0.0) for i in range(0, CHUNKS * BLOCK, per_rep)
                ], axis=0))
            picked = lax.dot_general(
                cut[side], jnp.concatenate(hot, axis=1).astype(jnp.bfloat16),
                (((1,), (0,)), ((), ())), preferred_element_type=jnp.float32,
            )
            picked = picked[: 3 * span] + picked[3 * span : 6 * span] + picked[6 * span :]
            for v in range(2):
                for c in range(3):
                    value = jnp.zeros((per_rep, BLOCK), jnp.float32)
                    for t in range(0, span, per_rep):
                        at = c * span + t
                        block = picked[at : at + per_rep, v * BLOCK : (v + 1) * BLOCK]
                        value = value + jnp.where(group[v] == t, block, 0.0)
                    part[k, c, s + v : s + v + 1, :] = jnp.sum(value, axis=0, keepdims=True)

    width = prod.shape[1]
    ones = jnp.ones((BLOCK, BLOCK), jnp.bfloat16)
    across = lax.broadcasted_iota(jnp.int32, (per_rep, BLOCK), 1) - sub

    def terms(k, q):
        p = [inbox[k, c * per_rep : (c + 1) * per_rep, :] for c in range(3)]
        m = [part[k, c] for c in range(3)]
        resid = m[0] * (p[0] - q[0]) + m[1] * (p[1] - q[1]) + m[2] * (p[2] - q[2])
        weight = 1.0 / (1.0 + resid * resid)
        jacob = [
            p[1] * m[2] - p[2] * m[1],
            p[2] * m[0] - p[0] * m[2],
            p[0] * m[1] - p[1] * m[0],
            m[0],
            m[1],
            m[2],
        ]
        for i in range(6):
            scaled = jacob[i] * weight
            for j in range(i, 6):
                line = jnp.sum(scaled * jacob[j], axis=0, keepdims=True)
                prod[k, 6 * i + j : 6 * i + j + 1, :] = line
                if j != i:
                    prod[k, 6 * j + i : 6 * j + i + 1, :] = line
            prod[k, 36 + i : 37 + i, :] = jnp.sum(scaled * resid, axis=0, keepdims=True)

    own_groups = n_own // GROUP
    groups = rounds // GROUP
    turns = jnp.logical_and(me < PLANE, own_groups == 0)
    early = PLANE - 1 - spot

    first_four = [early, GROUP + 1, GROUP, GROUP + 2]

    def work(ks, ready=0):
        for k in ks[ready:]:
            incoming(k).wait_recv()
        for i, k in enumerate(ks):
            side = jnp.where(k < n_own, 0, 1)
            look_up_normals(k, side)
            terms(k, [seen[k, c] for c in range(3)] if i < ready else points_of(k, side))
        for k in ks:
            left = prod[k]
            wide = jnp.zeros((width, BLOCK), jnp.float32)
            for _ in range(3):
                high = left.astype(jnp.bfloat16)
                wide = wide + jnp.dot(high, ones, preferred_element_type=jnp.float32)
                left = left - high.astype(jnp.float32)
            line = jnp.zeros((per_rep, BLOCK), jnp.float32)
            for t in range(0, width, per_rep):
                line = line + jnp.where(across == t, wide[t : t + per_rep], 0.0)
            line = jnp.sum(line, axis=0, keepdims=True)
            res[k] = line / (reps * per_rep * BLOCK)
        for k in ks:
            for r in range(reps):
                returned(k, r).start()

    deep = jnp.logical_and(turns, early >= 2)

    @pl.when(deep)
    def _():
        work([0, 1])

    def plain(g, carry):
        work([GROUP * g + u for u in range(GROUP)])
        return carry

    lax.fori_loop(0, own_groups, plain, 0)

    @pl.when(wraps)
    def _():
        def take(i):
            push(i).wait_recv()

            if i < final:

                @pl.when(lead)
                def _():
                    share(i).start()

        for i in range(CHUNKS):
            take(i)

        @pl.when(turns)
        def _():
            for k in first_four[:2]:
                incoming(k).wait_recv()
            for k in first_four[:2]:
                found = points_of(k, jnp.where(k < n_own, 0, 1))
                for c in range(3):
                    seen[k, c] = found[c]

        for i in range(CHUNKS, 2 * CHUNKS):
            take(i)
        split_table(1)

        @pl.when(turns)
        def _():
            others = [u + jnp.where(u >= early, 1, 0) for u in range(GROUP - 1)]

            @pl.when(deep)
            def _():
                work(first_four[:2], 2)
                work(first_four[2:] + [GROUP + 3, GROUP + 1 - early])

            @pl.when(jnp.logical_not(deep))
            def _():
                work(first_four[:2], 2)
                work(first_four[2:] + [GROUP + 3] + others)

        @pl.when(jnp.logical_not(turns))
        def _():
            lax.fori_loop(own_groups, groups, plain, 0)

    lanes = lax.broadcasted_iota(jnp.int32, (1, BLOCK), 1)
    sign = jnp.where(lanes < 36, 1.0, -1.0)
    total = jnp.zeros((1, BLOCK), jnp.float32)
    lower = jnp.zeros((1, BLOCK), jnp.float32)
    for k in range(rounds):
        mine = k < n_own
        total = total + jnp.where(mine, res[k], 0.0)
        lower = lower + jnp.where(mine, 0.0, res[k])
    own[...] = total * sign
    swap = pltpu.make_async_remote_copy(
        src_ref=own,
        dst_ref=other,
        send_sem=pair_send,
        recv_sem=pair_recv,
        device_id={"blk": me, "rep": partner},
        device_id_type=MESH,
    )
    swap.start()

    @pl.when(wraps)
    def _():
        low_sum[...] = lower * sign
        for r in range(reps):
            lowered(r).start()

    pltpu.make_async_remote_copy(
        src_ref=stage,
        dst_ref=inbox,
        send_sem=out_send,
        recv_sem=out_recv.at[0],
        device_id={"blk": above, "rep": half},
        device_id_type=MESH,
    ).wait_send()

    @pl.when(jnp.logical_and(wraps, lead))
    def _():
        pltpu.make_async_remote_copy(
            src_ref=tab,
            dst_ref=tab,
            send_sem=push_send,
            recv_sem=push_recv.at[0],
            device_id={"blk": above, "rep": half},
            device_id_type=MESH,
        ).wait_send()

    @pl.when(wraps)
    def _():
        raised().wait_send()

    arrivals().wait_send()
    swap.wait()
    total = own[...] + other[...]
    arrivals().wait_recv()
    for k in range(rounds):
        both = got[k, 0] + got[k, 1]
        out[k : k + 1, :] = both
        total = total + both
    own[...] = total

    @pl.when(wraps)
    def _():
        raised().wait_recv()
        own[...] = own[...] + high_sum[0] + high_sum[1]

    out[rounds : rounds + 1, :] = own[...] / (2.0 * rounds)


def split(sums, diag_ref, grad_ref, pair_ref):
    rounds = pair_ref.shape[0]
    for k in range(rounds):
        pair_ref[k, 0] = sums[k : k + 1, :36]
    diag_ref[...] = sums[rounds : rounds + 1, :36]
    grad_ref[...] = sums[rounds : rounds + 1, 36:42]


def by_rows(scan):
    return jnp.moveaxis(scan, 1, 0).reshape(scan.shape[1], -1, BLOCK)


def body(n, reps, points, normals, src_block, tgt_index, active):
    rounds, count = src_block.shape[:2]
    per_rep = src_block.shape[3]
    if count != 1 or reps != 2 or n % PLANE or n <= PLANE or rounds > PLANE // 2 or rounds != 2 * GROUP:
        raise ValueError("unsupported sizes")
    vmem = pl.BlockSpec(memory_space=pltpu.VMEM)
    f32, i32 = jnp.float32, jnp.int32
    rows = points.shape[2] // BLOCK
    dma = pltpu.SemaphoreType.DMA
    sums = pl.pallas_call(
        functools.partial(kernel, n, reps),
        out_shape=pltpu.VMEM((rounds + 1, BLOCK), f32),
        in_specs=[pl.BlockSpec(memory_space=pl.ANY)] * 5,
        out_specs=vmem,
        scratch_shapes=[
            pltpu.VMEM((3, rows, BLOCK), f32),
            pltpu.VMEM((2, CHUNKS, 6, rows // CHUNKS, BLOCK), f32),
            pltpu.VMEM((2, 9 * rows // CHUNKS, CHUNKS * BLOCK), jnp.bfloat16),
            pltpu.SMEM(src_block.shape, i32),
            pltpu.VMEM(tgt_index.shape, i32),
            pltpu.SMEM((1, rounds), i32),
            pltpu.VMEM((rounds, 4 * per_rep, BLOCK), f32),
            pltpu.VMEM((rounds, 4 * per_rep, BLOCK), f32),
            pltpu.VMEM((rounds, 3, per_rep, BLOCK), f32),
            pltpu.VMEM((rounds, 3, per_rep, BLOCK), f32),
            pltpu.VMEM((rounds, 48, BLOCK), f32),
            pltpu.VMEM((rounds, 1, BLOCK), f32),
            pltpu.VMEM((rounds, reps, 1, BLOCK), f32),
            pltpu.VMEM((1, BLOCK), f32),
            pltpu.VMEM((1, BLOCK), f32),
            pltpu.VMEM((1, BLOCK), f32),
            pltpu.VMEM((reps, 1, BLOCK), f32),
            dma((4,)),
            dma,
            dma,
            dma((rounds,)),
            dma,
            dma,
            dma,
            dma,
            dma,
            dma((2 * CHUNKS,)),
            dma,
            dma,
        ],
        compiler_params=pltpu.CompilerParams(collective_id=0, has_side_effects=True),
        name="normal_equations",
    )(by_rows(points), by_rows(normals), src_block, tgt_index, active.reshape(1, rounds))
    return pl.pallas_call(
        split,
        out_shape=(
            jax.ShapeDtypeStruct((1, 36), f32),
            jax.ShapeDtypeStruct((1, 6), f32),
            jax.ShapeDtypeStruct((rounds, 1, 1, 36), f32),
        ),
        in_specs=[vmem],
        out_specs=(vmem, vmem, vmem),
        name="split_sums",
    )(pltpu.with_memory_space_constraint(sums, pltpu.VMEM))


def solution(mesh):
    return jax.shard_map(
        functools.partial(body, mesh.shape["blk"], mesh.shape["rep"]),
        mesh=mesh,
        in_specs=(
            P("blk", None, None),
            P("blk", None, None),
            P(None, "blk", None, "rep"),
            P(None, "blk", None, "rep", None),
            P(None, "blk", None),
        ),
        out_specs=(P("blk", None), P("blk", None), P(None, "blk", None, None)),
        check_vma=False,
    )
```

```python
import functools

import jax
import jax.numpy as jnp
from jax import lax
from jax.experimental import pallas as pl
from jax.experimental.pallas import tpu as pltpu
from jax.sharding import PartitionSpec as P

BLOCK = 128
PLANE = 16
CHUNKS = 2
GROUP = 4
MESH = pl.DeviceIdType.MESH


def kernel(
    n, reps, pts_hbm, nrm_hbm, src_hbm, tgt_hbm, act_hbm, out,
    pts, tab, cut, src, tgt, act, stage, inbox, part, seen, prod, res, got, own, other, low_sum, high_sum,
    load, fill, out_send, out_recv, back_send, back_recv, pair_send, pair_recv,
    push_send, push_recv, low_send, low_recv,
):
    rounds, per_rep = tgt.shape[0], tgt.shape[3]
    rows = pts.shape[1]
    span = rows // CHUNKS
    npts = rows * BLOCK
    me = lax.axis_index("blk")
    half = lax.axis_index("rep")
    partner = 1 - half
    spot = lax.rem(me, PLANE)
    above = me + PLANE - jnp.where(me >= n - PLANE, n, 0)
    below = me - PLANE + jnp.where(me < PLANE, n, 0)
    wraps = spot >= PLANE - rounds
    lead = half == reps - 1
    n_own = jnp.minimum(rounds, PLANE - 1 - spot)

    def peer(d):
        return me + d - jnp.where(spot + d >= PLANE, PLANE, 0)

    sub = lax.broadcasted_iota(jnp.int32, (per_rep, BLOCK), 0)

    def split_table(side):
        for c in range(3):
            for chunk in range(CHUNKS):
                value = tab[side, chunk, 3 + c]
                lanes = slice(chunk * BLOCK, (chunk + 1) * BLOCK)
                for piece in range(3):
                    high = value.astype(jnp.bfloat16)
                    at = (3 * piece + c) * span
                    cut[side, at : at + span, lanes] = high
                    value = value - high.astype(jnp.float32)

    loads = [
        pltpu.make_async_copy(a, b, load.at[i])
        for i, (a, b) in enumerate(((src_hbm, src), (act_hbm, act), (tgt_hbm, tgt), (pts_hbm, pts)))
    ]
    fills = [
        pltpu.make_async_copy(
            a.at[:, c * span : (c + 1) * span, :], tab.at[0, c, 3 * i : 3 * i + 3], fill
        )
        for c in range(CHUNKS)
        for i, a in enumerate((pts_hbm, nrm_hbm))
    ]
    barrier = pltpu.get_barrier_semaphore()
    for d in (6, 7, 2, 5, 8, 3, 1, 4):
        pl.semaphore_signal(
            barrier, inc=1, device_id={"blk": peer(d), "rep": half}, device_id_type=MESH
        )
    pl.semaphore_signal(barrier, inc=1, device_id={"blk": me, "rep": partner}, device_id_type=MESH)
    pl.semaphore_signal(
        barrier, inc=1, device_id={"blk": below, "rep": reps - 1}, device_id_type=MESH
    )

    for copy in fills + loads:
        copy.start()

    prod[...] = jnp.zeros_like(prod)
    res[...] = jnp.zeros_like(res)
    pltpu.make_async_copy(tab.at[1], tab.at[0], fill).wait()

    pl.semaphore_wait(barrier, rounds + 1 + jnp.where(lead, reps, 0))

    def outgoing(k):
        return pltpu.make_async_remote_copy(
            src_ref=stage.at[k],
            dst_ref=inbox.at[k],
            send_sem=out_send,
            recv_sem=out_recv.at[k],
            device_id={"blk": peer(PLANE - 1 - k), "rep": half},
            device_id_type=MESH,
        )

    def incoming(k):
        return pltpu.make_async_remote_copy(
            src_ref=stage.at[0],
            dst_ref=inbox.at[k],
            send_sem=out_send,
            recv_sem=out_recv.at[k],
            device_id={"blk": above, "rep": half},
            device_id_type=MESH,
        )

    def returned(k, r):
        return pltpu.make_async_remote_copy(
            src_ref=res.at[k],
            dst_ref=got.at[k, half],
            send_sem=back_send,
            recv_sem=back_recv,
            device_id={"blk": peer(k + 1), "rep": r},
            device_id_type=MESH,
        )

    def arrivals():
        return pltpu.make_async_remote_copy(
            src_ref=got,
            dst_ref=got,
            send_sem=back_send,
            recv_sem=back_recv,
            device_id={"blk": above, "rep": half},
            device_id_type=MESH,
        )

    def piece(side, i):
        at = 3 * (i // CHUNKS)
        return tab.at[side, i % CHUNKS, at : at + 3]

    final = 2 * CHUNKS - 1

    def push(i, r=reps - 1):
        return pltpu.make_async_remote_copy(
            src_ref=piece(0, i),
            dst_ref=piece(1, i),
            send_sem=push_send,
            recv_sem=push_recv.at[i],
            device_id={"blk": above, "rep": r},
            device_id_type=MESH,
        )

    def share(i):
        return pltpu.make_async_remote_copy(
            src_ref=piece(1, i),
            dst_ref=piece(1, i),
            send_sem=push_send,
            recv_sem=push_recv.at[i],
            device_id={"blk": me, "rep": partner},
            device_id_type=MESH,
        )

    def lowered(r):
        return pltpu.make_async_remote_copy(
            src_ref=low_sum,
            dst_ref=high_sum.at[half],
            send_sem=low_send,
            recv_sem=low_recv,
            device_id={"blk": below, "rep": r},
            device_id_type=MESH,
        )

    def raised():
        return pltpu.make_async_remote_copy(
            src_ref=high_sum,
            dst_ref=high_sum,
            send_sem=low_send,
            recv_sem=low_recv,
            device_id={"blk": below, "rep": half},
            device_id_type=MESH,
        )

    @pl.when(jnp.logical_and(wraps, lead))
    def _():
        for i in range(final):
            push(i).start()
        for r in range(reps):
            push(final, r).start()

    for copy in loads:
        copy.wait()

    slot = lax.broadcasted_iota(jnp.int32, (per_rep, BLOCK), 0) + half * per_rep
    for k in range(rounds):
        for j in range(per_rep):
            block = src[k, 0, 0, j]
            for c in range(3):
                stage[k, c * per_rep + j, :] = pts[c, block]
        index = jnp.where(slot < act[0, k], tgt[k, 0, 0], npts)
        stage[k, 3 * per_rep :, :] = index.astype(jnp.float32)
    for k in range(rounds):
        outgoing(k).start()
    split_table(0)
    def points_of(k, side):
        index = inbox[k, 3 * per_rep :, :].astype(jnp.int32)
        lane = index & (BLOCK - 1)
        row = index >> (BLOCK.bit_length() - 1)
        found = [jnp.zeros((per_rep, BLOCK), jnp.float32) for c in range(3)]
        for chunk in range(CHUNKS):
            for h in range(span):
                here = row == chunk * span + h
                for c in range(3):
                    line = jnp.broadcast_to(tab[side, chunk, c, h : h + 1, :], (per_rep, BLOCK))
                    value = jnp.take_along_axis(line, lane, axis=1, mode="promise_in_bounds")
                    found[c] = jnp.where(here, value, found[c])
        return found

    def look_up_normals(k, side):
        for s in range(0, per_rep, 2):
            hot, group = [], []
            for v in range(2):
                at = 3 * per_rep + s + v
                line = jnp.broadcast_to(inbox[k, at : at + 1, :], (per_rep, BLOCK))
                line = line.astype(jnp.int32)
                row = line >> (BLOCK.bit_length() - 1)
                column = (line & (BLOCK - 1)) + (row >> (span.bit_length() - 1)) * BLOCK - sub
                group.append((row & (span - 1)) - sub)
                hot.append(jnp.concatenate([
                    jnp.where(column == i, 1.0, 0.0) for i in range(0, CHUNKS * BLOCK, per_rep)
                ], axis=0))
            picked = lax.dot_general(
                cut[side], jnp.concatenate(hot, axis=1).astype(jnp.bfloat16),
                (((1,), (0,)), ((), ())), preferred_element_type=jnp.float32,
            )
            picked = picked[: 3 * span] + picked[3 * span : 6 * span] + picked[6 * span :]
            for v in range(2):
                for c in range(3):
                    value = jnp.zeros((per_rep, BLOCK), jnp.float32)
                    for t in range(0, span, per_rep):
                        at = c * span + t
                        block = picked[at : at + per_rep, v * BLOCK : (v + 1) * BLOCK]
                        value = value + jnp.where(group[v] == t, block, 0.0)
                    part[k, c, s + v : s + v + 1, :] = jnp.sum(value, axis=0, keepdims=True)

    width = prod.shape[1]
    ones = jnp.ones((BLOCK, BLOCK), jnp.bfloat16)
    across = lax.broadcasted_iota(jnp.int32, (per_rep, BLOCK), 1) - sub

    def terms(k, q):
        p = [inbox[k, c * per_rep : (c + 1) * per_rep, :] for c in range(3)]
        m = [part[k, c] for c in range(3)]
        resid = m[0] * (p[0] - q[0]) + m[1] * (p[1] - q[1]) + m[2] * (p[2] - q[2])
        weight = 1.0 / (1.0 + resid * resid)
        jacob = [
            p[1] * m[2] - p[2] * m[1],
            p[2] * m[0] - p[0] * m[2],
            p[0] * m[1] - p[1] * m[0],
            m[0],
            m[1],
            m[2],
        ]
        for i in range(6):
            scaled = jacob[i] * weight
            for j in range(i, 6):
                line = jnp.sum(scaled * jacob[j], axis=0, keepdims=True)
                prod[k, 6 * i + j : 6 * i + j + 1, :] = line
                if j != i:
                    prod[k, 6 * j + i : 6 * j + i + 1, :] = line
            prod[k, 36 + i : 37 + i, :] = jnp.sum(scaled * resid, axis=0, keepdims=True)

    own_groups = n_own // GROUP
    groups = rounds // GROUP
    turns = jnp.logical_and(me < PLANE, own_groups == 0)
    early = PLANE - 1 - spot

    first_four = [early, GROUP + 1, GROUP, GROUP + 2]

    def work(ks, ready=0):
        for k in ks[ready:]:
            incoming(k).wait_recv()
        for i, k in enumerate(ks):
            side = jnp.where(k < n_own, 0, 1)
            look_up_normals(k, side)
            terms(k, [seen[k, c] for c in range(3)] if i < ready else points_of(k, side))
        for k in ks:
            left = prod[k]
            wide = jnp.zeros((width, BLOCK), jnp.float32)
            for _ in range(3):
                high = left.astype(jnp.bfloat16)
                wide = wide + jnp.dot(high, ones, preferred_element_type=jnp.float32)
                left = left - high.astype(jnp.float32)
            line = jnp.zeros((per_rep, BLOCK), jnp.float32)
            for t in range(0, width, per_rep):
                line = line + jnp.where(across == t, wide[t : t + per_rep], 0.0)
            line = jnp.sum(line, axis=0, keepdims=True)
            res[k] = line / (reps * per_rep * BLOCK)
        for k in ks:
            for r in range(reps):
                returned(k, r).start()

    deep = jnp.logical_and(turns, early >= 2)

    @pl.when(deep)
    def _():
        work([0, 1])

    def plain(g, carry):
        work([GROUP * g + u for u in range(GROUP)])
        return carry

    lax.fori_loop(0, own_groups, plain, 0)

    @pl.when(wraps)
    def _():
        def take(i):
            push(i).wait_recv()

            if i < final:

                @pl.when(lead)
                def _():
                    share(i).start()

        for i in range(CHUNKS):
            take(i)

        @pl.when(turns)
        def _():
            for k in first_four:
                incoming(k).wait_recv()
            for k in first_four:
                found = points_of(k, jnp.where(k < n_own, 0, 1))
                for c in range(3):
                    seen[k, c] = found[c]

        for i in range(CHUNKS, 2 * CHUNKS):
            take(i)
        split_table(1)

        @pl.when(turns)
        def _():
            others = [u + jnp.where(u >= early, 1, 0) for u in range(GROUP - 1)]

            @pl.when(deep)
            def _():
                work(first_four[:2], 2)
                work(first_four[2:] + [GROUP + 3, GROUP + 1 - early], 2)

            @pl.when(jnp.logical_not(deep))
            def _():
                work(first_four[:2], 2)
                work(first_four[2:] + [GROUP + 3] + others, 2)

        @pl.when(jnp.logical_not(turns))
        def _():
            lax.fori_loop(own_groups, groups, plain, 0)

    lanes = lax.broadcasted_iota(jnp.int32, (1, BLOCK), 1)
    sign = jnp.where(lanes < 36, 1.0, -1.0)
    total = jnp.zeros((1, BLOCK), jnp.float32)
    lower = jnp.zeros((1, BLOCK), jnp.float32)
    for k in range(rounds):
        mine = k < n_own
        total = total + jnp.where(mine, res[k], 0.0)
        lower = lower + jnp.where(mine, 0.0, res[k])
    own[...] = total * sign
    swap = pltpu.make_async_remote_copy(
        src_ref=own,
        dst_ref=other,
        send_sem=pair_send,
        recv_sem=pair_recv,
        device_id={"blk": me, "rep": partner},
        device_id_type=MESH,
    )
    swap.start()

    @pl.when(wraps)
    def _():
        low_sum[...] = lower * sign
        for r in range(reps):
            lowered(r).start()

    pltpu.make_async_remote_copy(
        src_ref=stage,
        dst_ref=inbox,
        send_sem=out_send,
        recv_sem=out_recv.at[0],
        device_id={"blk": above, "rep": half},
        device_id_type=MESH,
    ).wait_send()

    @pl.when(jnp.logical_and(wraps, lead))
    def _():
        pltpu.make_async_remote_copy(
            src_ref=tab,
            dst_ref=tab,
            send_sem=push_send,
            recv_sem=push_recv.at[0],
            device_id={"blk": above, "rep": half},
            device_id_type=MESH,
        ).wait_send()

    @pl.when(wraps)
    def _():
        raised().wait_send()

    arrivals().wait_send()
    swap.wait()
    total = own[...] + other[...]
    arrivals().wait_recv()
    for k in range(rounds):
        both = got[k, 0] + got[k, 1]
        out[k : k + 1, :] = both
        total = total + both
    own[...] = total

    @pl.when(wraps)
    def _():
        raised().wait_recv()
        own[...] = own[...] + high_sum[0] + high_sum[1]

    out[rounds : rounds + 1, :] = own[...] / (2.0 * rounds)


def split(sums, diag_ref, grad_ref, pair_ref):
    rounds = pair_ref.shape[0]
    for k in range(rounds):
        pair_ref[k, 0] = sums[k : k + 1, :36]
    diag_ref[...] = sums[rounds : rounds + 1, :36]
    grad_ref[...] = sums[rounds : rounds + 1, 36:42]


def by_rows(scan):
    return jnp.moveaxis(scan, 1, 0).reshape(scan.shape[1], -1, BLOCK)


def body(n, reps, points, normals, src_block, tgt_index, active):
    rounds, count = src_block.shape[:2]
    per_rep = src_block.shape[3]
    if count != 1 or reps != 2 or n % PLANE or n <= PLANE or rounds > PLANE // 2 or rounds != 2 * GROUP:
        raise ValueError("unsupported sizes")
    vmem = pl.BlockSpec(memory_space=pltpu.VMEM)
    f32, i32 = jnp.float32, jnp.int32
    rows = points.shape[2] // BLOCK
    dma = pltpu.SemaphoreType.DMA
    sums = pl.pallas_call(
        functools.partial(kernel, n, reps),
        out_shape=pltpu.VMEM((rounds + 1, BLOCK), f32),
        in_specs=[pl.BlockSpec(memory_space=pl.ANY)] * 5,
        out_specs=vmem,
        scratch_shapes=[
            pltpu.VMEM((3, rows, BLOCK), f32),
            pltpu.VMEM((2, CHUNKS, 6, rows // CHUNKS, BLOCK), f32),
            pltpu.VMEM((2, 9 * rows // CHUNKS, CHUNKS * BLOCK), jnp.bfloat16),
            pltpu.SMEM(src_block.shape, i32),
            pltpu.VMEM(tgt_index.shape, i32),
            pltpu.SMEM((1, rounds), i32),
            pltpu.VMEM((rounds, 4 * per_rep, BLOCK), f32),
            pltpu.VMEM((rounds, 4 * per_rep, BLOCK), f32),
            pltpu.VMEM((rounds, 3, per_rep, BLOCK), f32),
            pltpu.VMEM((rounds, 3, per_rep, BLOCK), f32),
            pltpu.VMEM((rounds, 48, BLOCK), f32),
            pltpu.VMEM((rounds, 1, BLOCK), f32),
            pltpu.VMEM((rounds, reps, 1, BLOCK), f32),
            pltpu.VMEM((1, BLOCK), f32),
            pltpu.VMEM((1, BLOCK), f32),
            pltpu.VMEM((1, BLOCK), f32),
            pltpu.VMEM((reps, 1, BLOCK), f32),
            dma((4,)),
            dma,
            dma,
            dma((rounds,)),
            dma,
            dma,
            dma,
            dma,
            dma,
            dma((2 * CHUNKS,)),
            dma,
            dma,
        ],
        compiler_params=pltpu.CompilerParams(collective_id=0, has_side_effects=True),
        name="normal_equations",
    )(by_rows(points), by_rows(normals), src_block, tgt_index, active.reshape(1, rounds))
    return pl.pallas_call(
        split,
        out_shape=(
            jax.ShapeDtypeStruct((1, 36), f32),
            jax.ShapeDtypeStruct((1, 6), f32),
            jax.ShapeDtypeStruct((rounds, 1, 1, 36), f32),
        ),
        in_specs=[vmem],
        out_specs=(vmem, vmem, vmem),
        name="split_sums",
    )(pltpu.with_memory_space_constraint(sums, pltpu.VMEM))


def solution(mesh):
    return jax.shard_map(
        functools.partial(body, mesh.shape["blk"], mesh.shape["rep"]),
        mesh=mesh,
        in_specs=(
            P("blk", None, None),
            P("blk", None, None),
            P(None, "blk", None, "rep"),
            P(None, "blk", None, "rep", None),
            P(None, "blk", None),
        ),
        out_specs=(P("blk", None), P("blk", None), P(None, "blk", None, None)),
        check_vma=False,
    )
```
